768 devices in a mesh: dom: 48 (over y_hi, z, core), grp: 16 (over x, y_lo).
Axes of the slice: x: 4, y: 8 (y_hi: 2, y_lo: 4; y = y_hi * 4 + y_lo), z: 12, core: 2. Of those that a mesh axis runs over, the one named last changes fastest.
Arguments:
- fine_level_residual: float32 [3, 15, 98304], P(None, None, ('dom', 'grp')), may hold values from -6 to 6
- restriction_matrix: float32 [3, 15], replicated, may hold values from -1.5 to 1.5
- prolongation_matrix: float32 [15, 3], replicated, may hold values from -3.5 to 3.5
- block_inverse: bfloat16 [9, 9, 98304], P(None, None, 'dom')
- face_coupling: bfloat16 [3, 9, 9, 98304], P(None, None, None, 'dom'), may hold values from -1.75 to 1.75
- neighbours: int32 [3, 98304], P(None, 'dom'), may hold values from -2048 to 2048, as said below
Outputs:
- correction: float32 [3, 15, 98304], P(None, None, ('dom', 'grp'))
The draws below stay inside these ranges and needn't reach their ends.
Inputs may be any that keep to these rules, and one draw needn't show every extreme that they name: `neighbours`: each entry is 0 or a nonzero offset d with |d| at most 2048 such that e + d is another triangle of the grid.
All inputs are finite; a program needn't handle non-finite values.
Results may differ from the reference program's by a relative error of at most 0.0003.
Values sent between devices are 32-bit elements; how exact they have to be, the bound alone decides.
A program may use at most 32 MiB of HBM per device.

```python
import jax
import jax.numpy as jnp
from jax import lax

EF = 128
SWEEPS = 6
ELEMS = 98304
N_GRP = 16


def draw_block_inverse(key, part):
    identity = jnp.eye(9, dtype=jnp.float32)[:, :, None]
    noise = jax.random.normal(jax.random.fold_in(key, 23), (9, 9, ELEMS), jnp.float32)
    value = 0.5 * identity + 0.08 * noise
    return value.astype(jnp.bfloat16)


def draw_neighbours(key, part):
    own = jnp.arange(ELEMS, dtype=jnp.int32)[None, :]
    reach = jax.random.randint(jax.random.fold_in(key, 31), (3, ELEMS), 1, EF * N_GRP + 1)
    direction = jax.random.randint(jax.random.fold_in(key, 32), (3, ELEMS), 0, 2) * 2 - 1
    offsets = reach * direction
    target = own + offsets
    wall = jax.random.randint(jax.random.fold_in(key, 33), (3, ELEMS), 0, 16) == 0
    inside = (target >= 0) & (target < ELEMS)
    return jnp.where(wall | jnp.logical_not(inside), 0, offsets).astype(jnp.int32)


def level_of(key, extent, shards, smallest, high):
    level = 1.0
    for dim, shards_of in shards:
        heights = jax.random.uniform(jax.random.fold_in(jax.random.fold_in(key, 6), dim), (shards_of,), jnp.float32, smallest / len(shards), high / len(shards))
        level = level * jnp.repeat(jnp.exp(heights), extent[dim] // shards_of).reshape((-1,) + (1,) * (len(extent) - 1 - dim))
    return level


def normal_values(key, shape, deviation, most, shards=(), kind=jnp.bfloat16):
    values = jax.random.normal(key, shape, jnp.float32) * deviation
    if len(shards) > 0:
        values = level_of(key, shape, shards, -0.22, 0.18) * values
    return jnp.clip(values, min=-most, max=most).astype(kind)


def setup_inputs(seed: int = 0) -> dict:
    keys = jax.random.split(jax.random.key(seed), 7)
    fine_level_residual = normal_values(keys[0], (3, 15, ELEMS), 1.0, 6.0, ((2, 768),), jnp.float32)
    restriction_matrix = normal_values(keys[1], (3, 15), 15 ** -0.5, 1.5, (), jnp.float32)
    prolongation_matrix = normal_values(keys[2], (15, 3), 3 ** -0.5, 3.5, (), jnp.float32)
    block_inverse = draw_block_inverse(jax.random.fold_in(keys[6], 71), 0)
    face_coupling = normal_values(keys[4], (3, 9, 9, ELEMS), 0.12, 1.75, ((3, 48),))
    neighbours = draw_neighbours(jax.random.fold_in(keys[6], 71), 0)
    return dict(fine_level_residual=fine_level_residual, restriction_matrix=restriction_matrix, prolongation_matrix=prolongation_matrix, block_inverse=block_inverse, face_coupling=face_coupling, neighbours=neighbours)


damping = 0.8


def one_sweep(current_iterate, coarse_forcing, block_inverse, face_coupling, neighbours):
    coupled = jnp.zeros_like(current_iterate)
    total = current_iterate.shape[1]
    own = jnp.arange(total, dtype=jnp.int32)
    for face_index in range(3):
        offsets = neighbours[face_index].astype(jnp.int32)
        position = jnp.clip(own + offsets, 0, total - 1).astype(jnp.int32)
        present = (offsets != 0).astype(jnp.float32)
        beside = current_iterate[:, position] * present[None, :]
        coupled = coupled + jnp.sum(face_coupling[face_index].astype(jnp.float32) * beside[None, :, :], axis=1)
    remain = coarse_forcing - coupled
    update = jnp.sum(block_inverse.astype(jnp.float32) * remain[None, :, :], axis=1)
    return (1.0 - damping) * current_iterate + damping * update


def reference(fine_level_residual, restriction_matrix, prolongation_matrix, block_inverse, face_coupling, neighbours):
    coarse_forcing = jnp.einsum("oc,acw->aow", restriction_matrix, fine_level_residual, precision=lax.Precision.HIGHEST)
    coarse_forcing = coarse_forcing.reshape(9, -1)
    current_iterate = jnp.zeros_like(coarse_forcing)
    for sweep_index in range(SWEEPS):
        current_iterate = one_sweep(current_iterate, coarse_forcing, block_inverse, face_coupling, neighbours)
    return jnp.einsum("oc,dcz->doz", prolongation_matrix, current_iterate.reshape(3, 3, -1), precision=lax.Precision.HIGHEST)
```

```python
import jax
import jax.numpy as jnp
from jax import lax
from jax.experimental import pallas as pl
from jax.experimental.pallas import tpu as pltpu
from jax.sharding import PartitionSpec as P

SWEEPS = 6
MESH = pl.DeviceIdType.MESH
damping = 0.8
N_GRP = 16
LANES = 128


def gathered(x, lane):
    return jnp.take_along_axis(x, lane, axis=1, mode="promise_in_bounds")


def kernel(
    n_dom,
    res_ref,
    rmat_ref,
    nb_ref,
    inv_hbm,
    cpl_hbm,
    out_ref,
    inv_v,
    cpl_v,
    dense,
    lane_idx,
    block_idx,
    own_rhs,
    land,
    rhs,
    table,
    beside,
    load_sem,
    gsend,
    grecv,
    hsend,
    hrecv,
):
    d = lax.axis_index("dom")
    g = lax.axis_index("grp")
    half = n_dom // 2
    mirror = (g // 4) * 4 + (3 - g % 4)
    low_g = jnp.where(d == half, mirror, g)
    high_g = jnp.where(d == half - 1, mirror, g)
    has_low = d > 0
    has_high = d < n_dom - 1

    barrier = pltpu.get_barrier_semaphore()
    for step in range(1, N_GRP):
        peer = lax.rem(g + step, N_GRP)
        pl.semaphore_signal(barrier, inc=1, device_id=(d, peer), device_id_type=MESH)

    @pl.when(has_low)
    def _():
        pl.semaphore_signal(barrier, inc=1, device_id=(d - 1, low_g), device_id_type=MESH)

    @pl.when(has_high)
    def _():
        pl.semaphore_signal(barrier, inc=1, device_id=(d + 1, high_g), device_id_type=MESH)

    load_inv = pltpu.make_async_copy(inv_hbm, inv_v, load_sem.at[0])
    load_cpl = pltpu.make_async_copy(cpl_hbm, cpl_v, load_sem.at[1])
    load_inv.start()
    load_cpl.start()

    for m in range(3):
        total = jnp.zeros((3, LANES), jnp.float32)
        for n in range(15):
            total = total + rmat_ref[m, n] * res_ref[:, n, :]
        for v in range(3):
            own_rhs[3 * v + m : 3 * v + m + 1, :] = total[v : v + 1, :]

    for f in range(3):
        for b in range(N_GRP):
            lane_idx[f, b : b + 1, :] = nb_ref[f : f + 1, b * LANES : (b + 1) * LANES]
        offsets = lane_idx[f]
        lanes = lax.broadcasted_iota(jnp.int32, (N_GRP, LANES), 1)
        column = offsets + lanes + N_GRP * LANES
        block_idx[f] = jnp.where(offsets != 0, lax.shift_right_arithmetic(column, 7), -1)
        lane_idx[f] = jnp.bitwise_and(column, LANES - 1)

    signals = N_GRP - 1 + has_low.astype(jnp.int32) + has_high.astype(jnp.int32)
    pl.semaphore_wait(barrier, signals)

    def rhs_copy(peer, source):
        return pltpu.make_async_remote_copy(
            src_ref=own_rhs,
            dst_ref=land.at[source],
            send_sem=gsend.at[peer],
            recv_sem=grecv.at[source],
            device_id=(d, peer),
            device_id_type=MESH,
        )

    for step in range(1, N_GRP):
        peer = lax.rem(g + step, N_GRP)
        rhs_copy(peer, g).start()

    load_inv.wait()

    def spread_inv(i, carry):
        for b in range(N_GRP):
            tile = inv_v[i, :, b * LANES : (b + 1) * LANES].astype(jnp.float32)
            dense[pl.ds(i * 144 + b, 9, stride=16), :] = tile
        return carry

    lax.fori_loop(0, 9, spread_inv, 0)
    load_cpl.wait()

    def spread_cpl(ij, carry):
        for b in range(N_GRP):
            tile = cpl_v[ij, :, b * LANES : (b + 1) * LANES].astype(jnp.float32)
            dense[pl.ds(1296 + ij * 16 + b, 3, stride=1296), :] = tile
        return carry

    lax.fori_loop(0, 81, spread_cpl, 0)

    land[g] = own_rhs[...]
    for step in range(1, N_GRP):
        peer = lax.rem(g + step, N_GRP)
        rhs_copy(peer, peer).wait_recv()
    for b in range(N_GRP):
        rhs[pl.ds(b, 9, stride=16), :] = land[b]

    def matrix(base, i, j, half_index):
        start = (base + i) * 144 + j * 16 + half_index * 8
        return dense[start : start + 8, :]

    def apply_inverse(remain, half_index):
        result = []
        for i in range(9):
            total = matrix(0, i, 0, half_index) * remain[0]
            for j in range(1, 9):
                total = total + matrix(0, i, j, half_index) * remain[j]
            result.append(total)
        return result

    for h in range(2):
        remain = [rhs[j * 16 + h * 8 : j * 16 + h * 8 + 8, :] for j in range(9)]
        for i, update in enumerate(apply_inverse(remain, h)):
            table[0, i, 16 + 8 * h : 24 + 8 * h, :] = damping * update

    def to_low(slot):
        return pltpu.make_async_remote_copy(
            src_ref=table.at[slot, :, 16:32, :],
            dst_ref=table.at[slot, :, 32:48, :],
            send_sem=hsend.at[slot, 0],
            recv_sem=hrecv.at[slot, 1],
            device_id=(d - 1, low_g),
            device_id_type=MESH,
        )

    def to_high(slot):
        return pltpu.make_async_remote_copy(
            src_ref=table.at[slot, :, 16:32, :],
            dst_ref=table.at[slot, :, 0:16, :],
            send_sem=hsend.at[slot, 1],
            recv_sem=hrecv.at[slot, 0],
            device_id=(d + 1, high_g),
            device_id_type=MESH,
        )

    def send(slot):
        @pl.when(has_low)
        def _():
            to_low(slot).start()

        @pl.when(has_high)
        def _():
            to_high(slot).start()

    send(0)

    def pick(slot, h, ks, resume):
        for f in range(3):
            lane = lane_idx[f, 8 * h : 8 * h + 8, :]
            block = block_idx[f, 8 * h : 8 * h + 8, :]
            masks = [block == k for k in ks]
            for v in range(9):
                if resume:
                    total = beside[f * 9 + v, 8 * h : 8 * h + 8, :]
                else:
                    total = jnp.zeros((8, LANES), jnp.float32)
                for k, mask in zip(ks, masks):
                    source = table[slot, v, 8 * h + k : 8 * h + k + 8, :]
                    total = jnp.where(mask, gathered(source, lane), total)
                beside[f * 9 + v, 8 * h : 8 * h + 8, :] = total

    def sweep(slot, carry):
        for h in range(2):
            pick(slot, h, range(16 - 8 * h, 25 - 8 * h), False)

        @pl.when(has_low)
        def _():
            to_high(slot).wait_recv()

        @pl.when(has_high)
        def _():
            to_low(slot).wait_recv()

        for h in range(2):
            ks = [k for k in range(33) if k < 16 - 8 * h or k >= 25 - 8 * h]
            pick(slot, h, ks, True)
            near = [beside[n, 8 * h : 8 * h + 8, :] for n in range(27)]
            remain = []
            for i in range(9):
                total = jnp.zeros((8, LANES), jnp.float32)
                for f in range(3):
                    for j in range(9):
                        total = total + matrix(9 + 9 * f, i, j, h) * near[9 * f + j]
                remain.append(rhs[i * 16 + h * 8 : i * 16 + h * 8 + 8, :] - total)
            for i, update in enumerate(apply_inverse(remain, h)):
                now = table[slot, i, 16 + 8 * h : 24 + 8 * h, :]
                table[slot + 1, i, 16 + 8 * h : 24 + 8 * h, :] = (
                    1.0 - damping
                ) * now + damping * update

        @pl.when(slot < SWEEPS - 2)
        def _():
            send(slot + 1)

        return carry

    lax.fori_loop(0, SWEEPS - 1, sweep, 0)

    for i in range(9):
        out_ref[i : i + 1, :] = table[SWEEPS - 1, i, pl.ds(16 + g, 1), :]

    for step in range(1, N_GRP):
        peer = lax.rem(g + step, N_GRP)
        rhs_copy(peer, g).wait_send()
    for slot in range(SWEEPS - 1):

        @pl.when(has_low)
        def _():
            to_low(slot).wait_send()

        @pl.when(has_high)
        def _():
            to_high(slot).wait_send()


def solution(mesh):
    n_dom = mesh.shape["dom"]

    def local(
        fine_level_residual,
        restriction_matrix,
        prolongation_matrix,
        block_inverse,
        face_coupling,
        neighbours,
    ):
        width = block_inverse.shape[2]
        call = pl.pallas_call(
            lambda *refs: kernel(n_dom, *refs),
            out_shape=jax.ShapeDtypeStruct((9, LANES), jnp.float32),
            in_specs=[
                pl.BlockSpec(memory_space=pltpu.VMEM),
                pl.BlockSpec(memory_space=pltpu.SMEM),
                pl.BlockSpec(memory_space=pltpu.VMEM),
                pl.BlockSpec(memory_space=pl.ANY),
                pl.BlockSpec(memory_space=pl.ANY),
            ],
            out_specs=pl.BlockSpec(memory_space=pltpu.VMEM),
            scratch_shapes=[
                pltpu.VMEM((9, 9, width), jnp.bfloat16),
                pltpu.VMEM((81, 3, width), jnp.bfloat16),
                pltpu.VMEM((36 * 144, LANES), jnp.float32),
                pltpu.VMEM((3, 16, LANES), jnp.int32),
                pltpu.VMEM((3, 16, LANES), jnp.int32),
                pltpu.VMEM((9, LANES), jnp.float32),
                pltpu.VMEM((16, 9, LANES), jnp.float32),
                pltpu.VMEM((144, LANES), jnp.float32),
                pltpu.VMEM((SWEEPS, 9, 48, LANES), jnp.float32),
                pltpu.VMEM((27, 16, LANES), jnp.float32),
                pltpu.SemaphoreType.DMA((2,)),
                pltpu.SemaphoreType.DMA((16,)),
                pltpu.SemaphoreType.DMA((16,)),
                pltpu.SemaphoreType.DMA((SWEEPS - 1, 2)),
                pltpu.SemaphoreType.DMA((SWEEPS - 1, 2)),
            ],
            compiler_params=pltpu.CompilerParams(collective_id=0, has_side_effects=True),
            name="jacobi",
        )
        iterate = call(
            fine_level_residual,
            restriction_matrix,
            neighbours,
            block_inverse,
            face_coupling.transpose(1, 2, 0, 3).reshape(81, 3, width),
        )
        parts = iterate.reshape(3, 3, LANES)
        return sum(
            prolongation_matrix[None, :, m, None] * parts[:, None, m, :] for m in range(3)
        )

    placed = (
        P(None, None, ("dom", "grp")),
        P(),
        P(),
        P(None, None, "dom"),
        P(None, None, None, "dom"),
        P(None, "dom"),
    )
    return jax.shard_map(
        local, mesh=mesh, in_specs=placed, out_specs=P(None, None, ("dom", "grp")), check_vma=False
    )
```

```python
import jax
import jax.numpy as jnp
from jax import lax
from jax.experimental import pallas as pl
from jax.experimental.pallas import tpu as pltpu
from jax.sharding import PartitionSpec as P

SWEEPS = 6
MESH = pl.DeviceIdType.MESH
damping = 0.8
N_GRP = 16
LANES = 128


def gathered(x, lane):
    return jnp.take_along_axis(x, lane, axis=1, mode="promise_in_bounds")


def kernel(
    n_dom,
    res_hbm,
    rmat_hbm,
    pmat_hbm,
    nb_hbm,
    inv_hbm,
    cpl_hbm,
    out_ref,
    res_ref,
    rmat_ref,
    pmat_ref,
    nb_ref,
    inv_v,
    cpl_v,
    dense,
    lane_idx,
    block_idx,
    own_rhs,
    land,
    rhs,
    table,
    beside,
    final,
    load_sem,
    gsend,
    grecv,
    hsend,
    hrecv,
):
    d = lax.axis_index("dom")
    g = lax.axis_index("grp")
    half = n_dom // 2
    column, row = g // 4 * 4, g % 4
    lead = jnp.logical_or(row == 0, row == 3)
    cross_low, cross_high = d == half, d == half - 1
    has = (d > 0, d < n_dom - 1)
    cross = (cross_low, cross_high)
    first_row = 3 - row
    second_row = jnp.where(row == 3, 1, 2)
    source_row = jnp.where(row < 2, 3, 0)
    side_dom = (d - 1, d + 1)
    first = [jnp.where(cross[s], column + first_row, g) for s in range(2)]
    second = column + second_row
    source = [jnp.where(cross[s], column + source_row, g) for s in range(2)]
    sends = [
        jnp.logical_and(has[s], jnp.logical_or(jnp.logical_not(cross[s]), lead)) for s in range(2)
    ]
    twice = [jnp.logical_and(cross[s], lead) for s in range(2)]

    barrier = pltpu.get_barrier_semaphore()
    for step in range(1, N_GRP):
        peer = lax.rem(g + step, N_GRP)
        pl.semaphore_signal(barrier, inc=1, device_id=(d, peer), device_id_type=MESH)
    for s in range(2):

        @pl.when(has[s])
        def _():
            pl.semaphore_signal(
                barrier, inc=1, device_id=(side_dom[s], source[s]), device_id_type=MESH
            )

    loads = [
        pltpu.make_async_copy(src, dst, load_sem.at[i])
        for i, (src, dst) in enumerate(
            (
                (res_hbm, res_ref),
                (rmat_hbm, rmat_ref),
                (pmat_hbm, pmat_ref),
                (nb_hbm, nb_ref),
                (inv_hbm, inv_v),
                (cpl_hbm, cpl_v),
            )
        )
    ]
    for load in loads:
        load.start()

    loads[0].wait()
    loads[1].wait()
    for m in range(3):
        total = jnp.zeros((3, LANES), jnp.float32)
        for n in range(15):
            total = total + rmat_ref[m, n] * res_ref[:, n, :]
        for v in range(3):
            own_rhs[3 * v + m : 3 * v + m + 1, :] = total[v : v + 1, :]

    signals = N_GRP - 1
    for flag in sends + twice:
        signals = signals + flag.astype(jnp.int32)
    pl.semaphore_wait(barrier, signals)

    def rhs_copy(peer, owner):
        return pltpu.make_async_remote_copy(
            src_ref=own_rhs,
            dst_ref=land.at[owner],
            send_sem=gsend.at[peer],
            recv_sem=grecv.at[owner],
            device_id=(d, peer),
            device_id_type=MESH,
        )

    for step in range(1, N_GRP):
        peer = lax.rem(g + step, N_GRP)
        rhs_copy(peer, g).start()

    loads[2].wait()
    loads[3].wait()
    for f in range(3):
        for b in range(N_GRP):
            lane_idx[f, b : b + 1, :] = nb_ref[f : f + 1, b * LANES : (b + 1) * LANES]
        offsets = lane_idx[f]
        lanes = lax.broadcasted_iota(jnp.int32, (N_GRP, LANES), 1)
        position = offsets + lanes + N_GRP * LANES
        block_idx[f] = jnp.where(offsets != 0, lax.shift_right_arithmetic(position, 7), -1)
        lane_idx[f] = jnp.bitwise_and(position, LANES - 1)

    loads[4].wait()

    def spread_inv(i, carry):
        for b in range(N_GRP):
            tile = inv_v[i, :, b * LANES : (b + 1) * LANES].astype(jnp.float32)
            dense[pl.ds(i * 144 + b, 9, stride=16), :] = tile
        return carry

    lax.fori_loop(0, 9, spread_inv, 0)
    loads[5].wait()

    def spread_cpl(ij, carry):
        for b in range(N_GRP):
            tile = cpl_v[ij, :, b * LANES : (b + 1) * LANES].astype(jnp.float32)
            dense[pl.ds(1296 + ij * 16 + b, 3, stride=1296), :] = tile
        return carry

    lax.fori_loop(0, 81, spread_cpl, 0)

    land[g] = own_rhs[...]
    for step in range(1, N_GRP):
        peer = lax.rem(g + step, N_GRP)
        rhs_copy(peer, peer).wait_recv()
    for b in range(N_GRP):
        rhs[pl.ds(b, 9, stride=16), :] = land[b]

    def matrix(base, i, j, h):
        start = (base + i) * 144 + j * 16 + h * 8
        return dense[pl.ds(start if isinstance(h, int) else pl.multiple_of(start, 8), 8), :]

    def apply_inverse(remain, h):
        result = [matrix(0, i, 0, h) * remain[0] for i in range(9)]
        for j in range(1, 9):
            result = [result[i] + matrix(0, i, j, h) * remain[j] for i in range(9)]
        return result

    for h in range(2):
        remain = [rhs[j * 16 + h * 8 : j * 16 + h * 8 + 8, :] for j in range(9)]
        for i, update in enumerate(apply_inverse(remain, h)):
            table[0, i, 16 + 8 * h : 24 + 8 * h, :] = damping * update

    def halo(slot, s, which, h):
        own, there = 16 + 8 * h, (32 if s == 0 else 0) + 8 * h
        return pltpu.make_async_remote_copy(
            src_ref=table.at[slot, :, own : own + 8, :],
            dst_ref=table.at[slot, :, there : there + 8, :],
            send_sem=hsend.at[slot, 4 * s + 2 * which + h],
            recv_sem=hrecv.at[slot, 2 * (1 - s) + h],
            device_id=(side_dom[s], second if which else first[s]),
            device_id_type=MESH,
        )

    def each_send(slot, act):
        for which, flags in ((0, sends), (1, twice)):
            for s in range(2):

                @pl.when(flags[s])
                def _():
                    act(halo(slot, s, which, s))
                    act(halo(slot, s, which, 1 - s))

    each_send(0, lambda copy: copy.start())

    def arrive(slot, s, far):
        for low in range(2):

            @pl.when(jnp.logical_and(s == low, has[low]))
            def _():
                halo(slot, 1 - low, 0, low if far else 1 - low).wait_recv()

    def pick(slot, h, start, k_start, count, resume):
        rows = pl.ds(pl.multiple_of(8 * h, 8), 8)
        for f in range(3):
            lane = lane_idx[f, rows, :]
            block = block_idx[f, rows, :] - k_start
            if resume:
                total = [beside[f * 9 + v, rows, :] for v in range(9)]
            else:
                total = [jnp.zeros((8, LANES), jnp.float32) for v in range(9)]
            for t in range(count):
                mask = block == t
                total = [
                    jnp.where(
                        mask,
                        gathered(table[slot, v, pl.ds(start + t, 8), :], lane),
                        total[v],
                    )
                    for v in range(9)
                ]
            for v in range(9):
                beside[f * 9 + v, rows, :] = total[v]

    def update(slot, h):
        rows = pl.ds(pl.multiple_of(8 * h, 8), 8)
        own = pl.ds(pl.multiple_of(16 + 8 * h, 8), 8)
        total = [jnp.zeros((8, LANES), jnp.float32) for i in range(9)]
        for f in range(3):
            for j in range(9):
                near = beside[f * 9 + j, rows, :]
                total = [total[i] + matrix(9 + 9 * f, i, j, h) * near for i in range(9)]
        remain = [
            rhs[pl.ds(pl.multiple_of(i * 16 + h * 8, 8), 8), :] - total[i] for i in range(9)
        ]
        for i, change in enumerate(apply_inverse(remain, h)):
            now = table[slot, i, own, :]
            table[slot + 1, i, own, :] = (1.0 - damping) * now + damping * change

    early = jnp.where(d < half, 0, 1)
    late = 1 - early

    def sweep(slot, carry):
        for h in range(2):
            pick(slot, h, 16, 16 - 8 * h, 9, False)
        for s in (early, late):
            arrive(slot, s, False)
            for h in range(2):
                pick(slot, h, 8 + 17 * s, 8 + 17 * s - 8 * h, 8, True)
            if s is late:
                update(slot, early)
            arrive(slot, s, True)
            pick(slot, s, 33 * s, 25 * s, 8, True)
        update(slot, late)

        @pl.when(slot < SWEEPS - 2)
        def _():
            each_send(slot + 1, lambda copy: copy.start())

        return carry

    lax.fori_loop(0, SWEEPS - 1, sweep, 0)

    for v in range(3):
        for m in range(3):
            final[m, v : v + 1, :] = table[SWEEPS - 1, 3 * v + m, pl.ds(16 + g, 1), :]
    coarse = [final[m, 0:3, :] for m in range(3)]
    for n in range(15):
        value = sum(pmat_ref[m, n] * coarse[m] for m in range(3))
        for v in range(3):
            out_ref[v, n : n + 1, :] = value[v : v + 1, :]

    for step in range(1, N_GRP):
        peer = lax.rem(g + step, N_GRP)
        rhs_copy(peer, g).wait_send()
    for slot in range(SWEEPS - 1):
        each_send(slot, lambda copy: copy.wait_send())


def solution(mesh):
    n_dom = mesh.shape["dom"]

    def local(
        fine_level_residual,
        restriction_matrix,
        prolongation_matrix,
        block_inverse,
        face_coupling,
        neighbours,
    ):
        width = block_inverse.shape[2]
        call = pl.pallas_call(
            lambda *refs: kernel(n_dom, *refs),
            out_shape=jax.ShapeDtypeStruct((3, 15, LANES), jnp.float32),
            in_specs=[pl.BlockSpec(memory_space=pl.ANY)] * 6,
            out_specs=pl.BlockSpec(memory_space=pltpu.VMEM),
            scratch_shapes=[
                pltpu.VMEM((3, 15, LANES), jnp.float32),
                pltpu.SMEM((3, 15), jnp.float32),
                pltpu.SMEM((3, 15), jnp.float32),
                pltpu.VMEM((3, width), jnp.int32),
                pltpu.VMEM((9, 9, width), jnp.bfloat16),
                pltpu.VMEM((81, 3, width), jnp.bfloat16),
                pltpu.VMEM((36 * 144, LANES), jnp.float32),
                pltpu.VMEM((3, 16, LANES), jnp.int32),
                pltpu.VMEM((3, 16, LANES), jnp.int32),
                pltpu.VMEM((9, LANES), jnp.float32),
                pltpu.VMEM((16, 9, LANES), jnp.float32),
                pltpu.VMEM((144, LANES), jnp.float32),
                pltpu.VMEM((SWEEPS, 9, 48, LANES), jnp.float32),
                pltpu.VMEM((27, 16, LANES), jnp.float32),
                pltpu.VMEM((3, 8, LANES), jnp.float32),
                pltpu.SemaphoreType.DMA((6,)),
                pltpu.SemaphoreType.DMA((16,)),
                pltpu.SemaphoreType.DMA((16,)),
                pltpu.SemaphoreType.DMA((SWEEPS - 1, 8)),
                pltpu.SemaphoreType.DMA((SWEEPS - 1, 4)),
            ],
            compiler_params=pltpu.CompilerParams(collective_id=0, has_side_effects=True),
            name="jacobi",
        )
        return call(
            fine_level_residual,
            restriction_matrix,
            prolongation_matrix.T,
            neighbours,
            block_inverse,
            face_coupling.transpose(1, 2, 0, 3).reshape(81, 3, width),
        )

    placed = (
        P(None, None, ("dom", "grp")),
        P(),
        P(),
        P(None, None, "dom"),
        P(None, None, None, "dom"),
        P(None, "dom"),
    )
    return jax.shard_map(
        local, mesh=mesh, in_specs=placed, out_specs=P(None, None, ("dom", "grp")), check_vma=False
    )
```

```python
import jax
import jax.numpy as jnp
from jax import lax
from jax.experimental import pallas as pl
from jax.experimental.pallas import tpu as pltpu
from jax.sharding import PartitionSpec as P

SWEEPS = 6
MESH = pl.DeviceIdType.MESH
damping = 0.8
N_GRP = 16
LANES = 128


def gathered(x, lane):
    return jnp.take_along_axis(x, lane, axis=1, mode="promise_in_bounds")


def kernel(
    n_dom,
    res_hbm,
    rmat_hbm,
    pmat_hbm,
    nb_hbm,
    inv_hbm,
    cpl_hbm,
    out_ref,
    res_ref,
    rmat_ref,
    pmat_ref,
    nb_ref,
    inv_v,
    cpl_v,
    dense,
    lane_idx,
    block_idx,
    own_rhs,
    land,
    rhs,
    table,
    beside,
    final,
    feed_own,
    feed,
    load_sem,
    gsend,
    grecv,
    hsend,
    hrecv,
    fsend,
    frecv,
):
    d = lax.axis_index("dom")
    g = lax.axis_index("grp")
    half = n_dom // 2
    column, row = g // 4 * 4, g % 4
    lead = jnp.logical_or(row == 0, row == 3)
    cross_low, cross_high = d == half, d == half - 1
    has = (d > 0, d < n_dom - 1)
    cross = (cross_low, cross_high)
    first_row = 3 - row
    second_row = jnp.where(row == 3, 1, 2)
    source_row = jnp.where(row < 2, 3, 0)
    side_dom = (d - 1, d + 1)
    first = [jnp.where(cross[s], column + first_row, g) for s in range(2)]
    second = column + second_row
    source = [jnp.where(cross[s], column + source_row, g) for s in range(2)]
    sends = [
        jnp.logical_and(has[s], jnp.logical_or(jnp.logical_not(cross[s]), lead)) for s in range(2)
    ]
    twice = [jnp.logical_and(cross[s], lead) for s in range(2)]
    feeding, fed = cross_high, jnp.logical_and(cross_low, lead)
    leads = [4 * x + y for x in range(4) for y in (3, 0)]

    barrier = pltpu.get_barrier_semaphore()
    for step in range(1, N_GRP):
        peer = lax.rem(g + step, N_GRP)
        pl.semaphore_signal(barrier, inc=1, device_id=(d, peer), device_id_type=MESH)
    for s in range(2):

        @pl.when(has[s] if s else jnp.logical_and(has[s], jnp.logical_not(fed)))
        def _():
            pl.semaphore_signal(
                barrier, inc=1, device_id=(side_dom[s], source[s]), device_id_type=MESH
            )

    @pl.when(fed)
    def _():
        for other in range(N_GRP):
            pl.semaphore_signal(barrier, inc=1, device_id=(d - 1, other), device_id_type=MESH)

    loads = [
        pltpu.make_async_copy(src, dst, load_sem.at[i])
        for i, (src, dst) in enumerate(
            (
                (res_hbm, res_ref),
                (rmat_hbm, rmat_ref),
                (pmat_hbm, pmat_ref),
                (nb_hbm, nb_ref),
                (inv_hbm, inv_v),
                (cpl_hbm, cpl_v),
            )
        )
    ]
    for load in loads:
        load.start()

    loads[0].wait()
    loads[1].wait()
    for m in range(3):
        total = jnp.zeros((3, LANES), jnp.float32)
        for n in range(15):
            total = total + rmat_ref[m, n] * res_ref[:, n, :]
        for v in range(3):
            own_rhs[3 * v + m : 3 * v + m + 1, :] = total[v : v + 1, :]

    signals = N_GRP - 1
    for flag in [sends[0]] + twice:
        signals = signals + flag.astype(jnp.int32)
    signals = signals + jnp.where(feeding, len(leads), sends[1].astype(jnp.int32))
    pl.semaphore_wait(barrier, signals)

    def rhs_copy(peer, owner):
        return pltpu.make_async_remote_copy(
            src_ref=own_rhs,
            dst_ref=land.at[owner],
            send_sem=gsend.at[peer],
            recv_sem=grecv.at[owner],
            device_id=(d, peer),
            device_id_type=MESH,
        )

    for step in range(1, N_GRP):
        peer = lax.rem(g + step, N_GRP)
        rhs_copy(peer, g).start()

    loads[4].wait()

    def feed_copy(k, owner):
        return pltpu.make_async_remote_copy(
            src_ref=feed_own,
            dst_ref=feed.at[owner],
            send_sem=fsend.at[k],
            recv_sem=frecv.at[owner],
            device_id=(d + 1, leads[k]),
            device_id_type=MESH,
        )

    @pl.when(feeding)
    def _():
        own = pl.ds(pl.multiple_of(g * LANES, LANES), LANES)
        for i in range(9):
            part = inv_v[i, :, own].astype(jnp.float32) * own_rhs[...]
            feed_own[i : i + 1, :] = damping * jnp.sum(part, axis=0, keepdims=True)
        for k in range(len(leads)):
            feed_copy(k, g).start()

    loads[2].wait()
    loads[3].wait()
    for f in range(3):
        for b in range(N_GRP):
            lane_idx[f, b : b + 1, :] = nb_ref[f : f + 1, b * LANES : (b + 1) * LANES]
        offsets = lane_idx[f]
        lanes = lax.broadcasted_iota(jnp.int32, (N_GRP, LANES), 1)
        position = offsets + lanes + N_GRP * LANES
        block_idx[f] = jnp.where(offsets != 0, lax.shift_right_arithmetic(position, 7), -1)
        lane_idx[f] = jnp.bitwise_and(position, LANES - 1)


    def spread_inv(i, carry):
        for b in range(N_GRP):
            tile = inv_v[i, :, b * LANES : (b + 1) * LANES].astype(jnp.float32)
            dense[pl.ds(i * 144 + b, 9, stride=16), :] = tile
        return carry

    lax.fori_loop(0, 9, spread_inv, 0)
    loads[5].wait()

    def spread_cpl(ij, carry):
        for b in range(N_GRP):
            tile = cpl_v[ij, :, b * LANES : (b + 1) * LANES].astype(jnp.float32)
            dense[pl.ds(1296 + ij * 16 + b, 3, stride=1296), :] = tile
        return carry

    lax.fori_loop(0, 81, spread_cpl, 0)

    land[g] = own_rhs[...]
    for step in range(1, N_GRP):
        peer = lax.rem(g + step, N_GRP)
        rhs_copy(peer, peer).wait_recv()
    for b in range(N_GRP):
        rhs[pl.ds(b, 9, stride=16), :] = land[b]

    def matrix(base, i, j, h):
        start = (base + i) * 144 + j * 16 + h * 8
        return dense[pl.ds(start if isinstance(h, int) else pl.multiple_of(start, 8), 8), :]

    def apply_inverse(remain, h):
        result = [matrix(0, i, 0, h) * remain[0] for i in range(9)]
        for j in range(1, 9):
            result = [result[i] + matrix(0, i, j, h) * remain[j] for i in range(9)]
        return result

    for h in range(2):
        remain = [rhs[j * 16 + h * 8 : j * 16 + h * 8 + 8, :] for j in range(9)]
        for i, update in enumerate(apply_inverse(remain, h)):
            table[0, i, 16 + 8 * h : 24 + 8 * h, :] = damping * update

    def halo(slot, s, which, h):
        own, there = 16 + 8 * h, (32 if s == 0 else 0) + 8 * h
        return pltpu.make_async_remote_copy(
            src_ref=table.at[slot, :, own : own + 8, :],
            dst_ref=table.at[slot, :, there : there + 8, :],
            send_sem=hsend.at[slot, 4 * s + 2 * which + h],
            recv_sem=hrecv.at[slot, 2 * (1 - s) + h],
            device_id=(side_dom[s], second if which else first[s]),
            device_id_type=MESH,
        )

    def each_send(slot, act, inner_first=False):
        order = ((0, sends), (1, twice))
        for which, flags in order[::-1] if inner_first else order:
            for s in range(2):
                flag = flags[s]
                if isinstance(slot, int) and slot == 0 and s == 1 and which == 0:
                    flag = jnp.logical_and(flag, jnp.logical_not(feeding))

                @pl.when(flag)
                def _():
                    act(halo(slot, s, which, s))
                    act(halo(slot, s, which, 1 - s))

    each_send(0, lambda copy: copy.start())

    def arrive(slot, s, far):
        for low in range(2):

            due = jnp.logical_and(s == low, has[low])
            if low == 0 and not isinstance(slot, int):
                due = jnp.logical_and(due, jnp.logical_not(jnp.logical_and(fed, slot == 0)))

            @pl.when(due)
            def _():
                halo(slot, 1 - low, 0, low if far else 1 - low).wait_recv()

    def pick(slot, h, start, k_start, count, resume):
        rows = pl.ds(pl.multiple_of(8 * h, 8), 8)
        for f in range(3):
            lane = lane_idx[f, rows, :]
            block = block_idx[f, rows, :] - k_start
            if resume:
                total = [beside[f * 9 + v, rows, :] for v in range(9)]
            else:
                total = [jnp.zeros((8, LANES), jnp.float32) for v in range(9)]
            for t in range(count):
                mask = block == t
                total = [
                    jnp.where(
                        mask,
                        gathered(table[slot, v, pl.ds(start + t, 8), :], lane),
                        total[v],
                    )
                    for v in range(9)
                ]
            for v in range(9):
                beside[f * 9 + v, rows, :] = total[v]

    def update(slot, h):
        rows = pl.ds(pl.multiple_of(8 * h, 8), 8)
        own = pl.ds(pl.multiple_of(16 + 8 * h, 8), 8)
        total = [jnp.zeros((8, LANES), jnp.float32) for i in range(9)]
        for f in range(3):
            for j in range(9):
                near = beside[f * 9 + j, rows, :]
                total = [total[i] + matrix(9 + 9 * f, i, j, h) * near for i in range(9)]
        remain = [
            rhs[pl.ds(pl.multiple_of(i * 16 + h * 8, 8), 8), :] - total[i] for i in range(9)
        ]
        for i, change in enumerate(apply_inverse(remain, h)):
            now = table[slot, i, own, :]
            table[slot + 1, i, own, :] = (1.0 - damping) * now + damping * change

    early = jnp.where(d < half, 0, 1)
    late = 1 - early

    def sweep(slot, carry):
        for h in range(2):
            pick(slot, h, 16, 16 - 8 * h, 9, False)
        for s in (early, late):
            if s is late:

                @pl.when(jnp.logical_and(fed, slot == 0))
                def _():
                    for b in range(N_GRP):
                        feed_copy(0, b).wait_recv()
                    for b in range(N_GRP):
                        for v in range(9):
                            table[0, v, b : b + 1, :] = feed[b, v : v + 1, :]

            arrive(slot, s, False)
            for h in range(2):
                pick(slot, h, 8 + 17 * s, 8 + 17 * s - 8 * h, 8, True)
            if s is late:
                update(slot, early)
            arrive(slot, s, True)
            pick(slot, s, 33 * s, 25 * s, 8, True)
        update(slot, late)

        @pl.when(slot < SWEEPS - 3)
        def _():
            each_send(slot + 1, lambda copy: copy.start())

        @pl.when(slot == SWEEPS - 3)
        def _():
            each_send(slot + 1, lambda copy: copy.start(), True)

        return carry

    lax.fori_loop(0, SWEEPS - 2, sweep, 0)

    last = SWEEPS - 2
    sublane = lax.broadcasted_iota(jnp.int32, (8, LANES), 0)
    mine = pl.ds(g, 1)

    def pick_last(tiles, resume):
        for f in range(3):
            lane = jnp.broadcast_to(lane_idx[f, mine, :], (8, LANES))
            block = jnp.broadcast_to(block_idx[f, mine, :], (8, LANES))
            block = jnp.where(block < 0, -1, block + g - sublane)
            if resume:
                total = [beside[f * 9 + v, 0:8, :] for v in range(9)]
            else:
                total = [jnp.zeros((8, LANES), jnp.float32) for v in range(9)]
            for tile in tiles:
                rows = pl.ds(pl.multiple_of(8 * tile, 8), 8)
                mask = block == 8 * tile
                total = [
                    jnp.where(mask, gathered(table[last, v, rows, :], lane), total[v])
                    for v in range(9)
                ]
            for v in range(9):
                beside[f * 9 + v, 0:8, :] = total[v]

    pick_last((2, 3), False)
    for v in range(9):
        final[0, v : v + 1, :] = table[last, v, pl.ds(16 + g, 1), :]
    for s in (early, late):
        arrive(last, s, False)
        pick_last((1 + 3 * s,), True)
        arrive(last, s, True)
        pick_last((5 * s,), True)
    coupled = jnp.zeros((9, LANES), jnp.float32)
    for f in range(3):
        for j in range(9):
            near = jnp.sum(beside[f * 9 + j, 0:8, :], axis=0, keepdims=True)
            coupled = coupled + dense[pl.ds((9 + 9 * f) * 144 + j * 16 + g, 9, stride=144), :] * near
    final[1, 0:9, :] = rhs[pl.ds(g, 9, stride=16), :] - coupled
    change = jnp.zeros((9, LANES), jnp.float32)
    for j in range(9):
        change = change + dense[pl.ds(j * 16 + g, 9, stride=144), :] * final[1, j : j + 1, :]
    final[2, 0:9, :] = (1.0 - damping) * final[0, 0:9, :] + damping * change
    coarse = [final[2, pl.ds(m, 3, stride=3), :] for m in range(3)]
    for n in range(15):
        value = sum(pmat_ref[m, n] * coarse[m] for m in range(3))
        for v in range(3):
            out_ref[v, n : n + 1, :] = value[v : v + 1, :]

    for step in range(1, N_GRP):
        peer = lax.rem(g + step, N_GRP)
        rhs_copy(peer, g).wait_send()
    for slot in range(SWEEPS - 1):
        each_send(slot, lambda copy: copy.wait_send())

    @pl.when(feeding)
    def _():
        for k in range(len(leads)):
            feed_copy(k, g).wait_send()


def solution(mesh):
    n_dom = mesh.shape["dom"]

    def local(
        fine_level_residual,
        restriction_matrix,
        prolongation_matrix,
        block_inverse,
        face_coupling,
        neighbours,
    ):
        width = block_inverse.shape[2]
        call = pl.pallas_call(
            lambda *refs: kernel(n_dom, *refs),
            out_shape=jax.ShapeDtypeStruct((3, 15, LANES), jnp.float32),
            in_specs=[pl.BlockSpec(memory_space=pl.ANY)] * 6,
            out_specs=pl.BlockSpec(memory_space=pltpu.VMEM),
            scratch_shapes=[
                pltpu.VMEM((3, 15, LANES), jnp.float32),
                pltpu.SMEM((3, 15), jnp.float32),
                pltpu.SMEM((3, 15), jnp.float32),
                pltpu.VMEM((3, width), jnp.int32),
                pltpu.VMEM((9, 9, width), jnp.bfloat16),
                pltpu.VMEM((81, 3, width), jnp.bfloat16),
                pltpu.VMEM((36 * 144, LANES), jnp.float32),
                pltpu.VMEM((3, 16, LANES), jnp.int32),
                pltpu.VMEM((3, 16, LANES), jnp.int32),
                pltpu.VMEM((9, LANES), jnp.float32),
                pltpu.VMEM((16, 9, LANES), jnp.float32),
                pltpu.VMEM((144, LANES), jnp.float32),
                pltpu.VMEM((SWEEPS - 1, 9, 48, LANES), jnp.float32),
                pltpu.VMEM((27, 16, LANES), jnp.float32),
                pltpu.VMEM((3, 16, LANES), jnp.float32),
                pltpu.VMEM((9, LANES), jnp.float32),
                pltpu.VMEM((16, 9, LANES), jnp.float32),
                pltpu.SemaphoreType.DMA((6,)),
                pltpu.SemaphoreType.DMA((16,)),
                pltpu.SemaphoreType.DMA((16,)),
                pltpu.SemaphoreType.DMA((SWEEPS - 1, 8)),
                pltpu.SemaphoreType.DMA((SWEEPS - 1, 4)),
                pltpu.SemaphoreType.DMA((8,)),
                pltpu.SemaphoreType.DMA((16,)),
            ],
            compiler_params=pltpu.CompilerParams(collective_id=0, has_side_effects=True),
            name="jacobi",
        )
        return call(
            fine_level_residual,
            restriction_matrix,
            prolongation_matrix.T,
            neighbours,
            block_inverse,
            face_coupling.transpose(1, 2, 0, 3).reshape(81, 3, width),
        )

    placed = (
        P(None, None, ("dom", "grp")),
        P(),
        P(),
        P(None, None, "dom"),
        P(None, None, None, "dom"),
        P(None, "dom"),
    )
    return jax.shard_map(
        local, mesh=mesh, in_specs=placed, out_specs=P(None, None, ("dom", "grp")), check_vma=False
    )
```

```python
import jax
import jax.numpy as jnp
from jax import lax
from jax.experimental import pallas as pl
from jax.experimental.pallas import tpu as pltpu
from jax.sharding import PartitionSpec as P

SWEEPS = 6
MESH = pl.DeviceIdType.MESH
damping = 0.8
N_GRP = 16
LANES = 128


def gathered(x, lane):
    return jnp.take_along_axis(x, lane, axis=1, mode="promise_in_bounds")


def kernel(
    n_dom,
    res_hbm,
    rmat_hbm,
    pmat_hbm,
    nb_hbm,
    inv_hbm,
    cpl_hbm,
    out_ref,
    res_ref,
    rmat_ref,
    pmat_ref,
    nb_ref,
    inv_v,
    cpl_v,
    dense,
    lane_idx,
    block_idx,
    own_rhs,
    land,
    rhs,
    table,
    beside,
    final,
    feed_own,
    feed,
    load_sem,
    gsend,
    grecv,
    hsend,
    hrecv,
    fsend,
    frecv,
    ready,
):
    d = lax.axis_index("dom")
    g = lax.axis_index("grp")
    half = n_dom // 2
    column, row = g // 4 * 4, g % 4
    lead = jnp.logical_or(row == 0, row == 3)
    cross_low, cross_high = d == half, d == half - 1
    has = (d > 0, d < n_dom - 1)
    cross = (cross_low, cross_high)
    first_row = 3 - row
    second_row = jnp.where(row == 3, 1, 2)
    source_row = jnp.where(row < 2, 3, 0)
    side_dom = (d - 1, d + 1)
    first = [jnp.where(cross[s], column + first_row, g) for s in range(2)]
    second = column + second_row
    source = [jnp.where(cross[s], column + source_row, g) for s in range(2)]
    sends = [
        jnp.logical_and(has[s], jnp.logical_or(jnp.logical_not(cross[s]), lead)) for s in range(2)
    ]
    twice = [jnp.logical_and(cross[s], lead) for s in range(2)]
    feeding, fed = cross_high, jnp.logical_and(cross_low, lead)
    leads = [4 * x + y for x in range(4) for y in (3, 0)]

    barrier = pltpu.get_barrier_semaphore()
    for step in range(1, N_GRP):
        peer = lax.rem(g + step, N_GRP)
        pl.semaphore_signal(barrier, inc=1, device_id=(d, peer), device_id_type=MESH)
    for s in range(2):

        @pl.when(jnp.logical_and(has[s], jnp.logical_not(feeding if s else fed)))
        def _():
            pl.semaphore_signal(
                barrier, inc=1, device_id=(side_dom[s], source[s]), device_id_type=MESH
            )

    @pl.when(fed)
    def _():
        for other in range(N_GRP):
            pl.semaphore_signal(barrier, inc=1, device_id=(d - 1, other), device_id_type=MESH)

    loads = [
        pltpu.make_async_copy(src, dst, load_sem.at[i])
        for i, (src, dst) in enumerate(
            (
                (res_hbm, res_ref),
                (rmat_hbm, rmat_ref),
                (pmat_hbm, pmat_ref),
                (nb_hbm, nb_ref),
                (inv_hbm, inv_v),
                (cpl_hbm, cpl_v),
            )
        )
    ]
    for load in loads:
        load.start()

    loads[0].wait()
    loads[1].wait()
    for m in range(3):
        total = jnp.zeros((3, LANES), jnp.float32)
        for n in range(15):
            total = total + rmat_ref[m, n] * res_ref[:, n, :]
        for v in range(3):
            own_rhs[3 * v + m : 3 * v + m + 1, :] = total[v : v + 1, :]

    signals = N_GRP - 1
    low = jnp.logical_and(sends[0], jnp.logical_not(cross_low))
    signals = signals + low.astype(jnp.int32) + twice[1].astype(jnp.int32)
    signals = signals + jnp.where(feeding, len(leads), sends[1].astype(jnp.int32))
    pl.semaphore_wait(barrier, signals)

    @pl.when(feeding)
    def _():
        pl.semaphore_signal(
            ready, inc=1, device_id=(side_dom[1], source[1]), device_id_type=MESH
        )

    def rhs_copy(peer, owner):
        return pltpu.make_async_remote_copy(
            src_ref=own_rhs,
            dst_ref=land.at[owner],
            send_sem=gsend.at[peer],
            recv_sem=grecv.at[owner],
            device_id=(d, peer),
            device_id_type=MESH,
        )

    for step in range(1, N_GRP):
        peer = lax.rem(g + step, N_GRP)
        rhs_copy(peer, g).start()

    loads[4].wait()

    def feed_copy(k, owner):
        return pltpu.make_async_remote_copy(
            src_ref=feed_own,
            dst_ref=feed.at[owner],
            send_sem=fsend.at[k],
            recv_sem=frecv.at[owner],
            device_id=(d + 1, leads[k]),
            device_id_type=MESH,
        )

    @pl.when(feeding)
    def _():
        own = pl.ds(pl.multiple_of(g * LANES, LANES), LANES)
        for i in range(9):
            part = inv_v[i, :, own].astype(jnp.float32) * own_rhs[...]
            feed_own[i : i + 1, :] = damping * jnp.sum(part, axis=0, keepdims=True)
        for k in range(len(leads)):
            feed_copy(k, g).start()

    loads[2].wait()
    loads[3].wait()
    for f in range(3):
        for b in range(N_GRP):
            lane_idx[f, b : b + 1, :] = nb_ref[f : f + 1, b * LANES : (b + 1) * LANES]
        offsets = lane_idx[f]
        lanes = lax.broadcasted_iota(jnp.int32, (N_GRP, LANES), 1)
        position = offsets + lanes + N_GRP * LANES
        block_idx[f] = jnp.where(offsets != 0, lax.shift_right_arithmetic(position, 7), -1)
        lane_idx[f] = jnp.bitwise_and(position, LANES - 1)


    def spread_inv(i, carry):
        for b in range(N_GRP):
            tile = inv_v[i, :, b * LANES : (b + 1) * LANES].astype(jnp.float32)
            dense[pl.ds(i * 144 + b, 9, stride=16), :] = tile
        return carry

    lax.fori_loop(0, 9, spread_inv, 0)
    loads[5].wait()

    def spread_cpl(ij, carry):
        for b in range(N_GRP):
            tile = cpl_v[ij, :, b * LANES : (b + 1) * LANES].astype(jnp.float32)
            dense[pl.ds(1296 + ij * 16 + b, 3, stride=1296), :] = tile
        return carry

    lax.fori_loop(0, 81, spread_cpl, 0)

    land[g] = own_rhs[...]
    for step in range(1, N_GRP):
        peer = lax.rem(g + step, N_GRP)
        rhs_copy(peer, peer).wait_recv()
    for b in range(N_GRP):
        rhs[pl.ds(b, 9, stride=16), :] = land[b]

    def matrix(base, i, j, h):
        start = (base + i) * 144 + j * 16 + h * 8
        return dense[pl.ds(start if isinstance(h, int) else pl.multiple_of(start, 8), 8), :]

    def apply_inverse(remain, h):
        result = [matrix(0, i, 0, h) * remain[0] for i in range(9)]
        for j in range(1, 9):
            result = [result[i] + matrix(0, i, j, h) * remain[j] for i in range(9)]
        return result

    for h in range(2):
        remain = [rhs[j * 16 + h * 8 : j * 16 + h * 8 + 8, :] for j in range(9)]
        for i, update in enumerate(apply_inverse(remain, h)):
            table[0, i, 16 + 8 * h : 24 + 8 * h, :] = damping * update

    def halo(slot, s, which, h):
        own, there = 16 + 8 * h, (32 if s == 0 else 0) + 8 * h
        return pltpu.make_async_remote_copy(
            src_ref=table.at[slot, :, own : own + 8, :],
            dst_ref=table.at[slot, :, there : there + 8, :],
            send_sem=hsend.at[slot, 4 * s + 2 * which + h],
            recv_sem=hrecv.at[slot, 2 * (1 - s) + h],
            device_id=(side_dom[s], second if which else first[s]),
            device_id_type=MESH,
        )

    def each_send(slot, act, inner_first=False, sides=(0, 1)):
        order = ((0, sends), (1, twice))
        for which, flags in order[::-1] if inner_first else order:
            for s in sides:
                flag = flags[s]
                if isinstance(slot, int) and slot == 0 and s == 1 and which == 0:
                    flag = jnp.logical_and(flag, jnp.logical_not(feeding))

                @pl.when(flag)
                def _():
                    act(halo(slot, s, which, s))
                    act(halo(slot, s, which, 1 - s))

    each_send(0, lambda copy: copy.start(), sides=(1,))

    @pl.when(fed)
    def _():
        pl.semaphore_wait(ready, 2)

    each_send(0, lambda copy: copy.start(), sides=(0,))

    def arrive(slot, s, far):
        for low in range(2):

            due = jnp.logical_and(s == low, has[low])
            if low == 0 and not isinstance(slot, int):
                due = jnp.logical_and(due, jnp.logical_not(jnp.logical_and(fed, slot == 0)))

            @pl.when(due)
            def _():
                halo(slot, 1 - low, 0, low if far else 1 - low).wait_recv()

    def pick(slot, h, start, k_start, count, resume):
        rows = pl.ds(pl.multiple_of(8 * h, 8), 8)
        for f in range(3):
            lane = lane_idx[f, rows, :]
            block = block_idx[f, rows, :] - k_start
            if resume:
                total = [beside[f * 9 + v, rows, :] for v in range(9)]
            else:
                total = [jnp.zeros((8, LANES), jnp.float32) for v in range(9)]
            for t in range(count):
                mask = block == t
                total = [
                    jnp.where(
                        mask,
                        gathered(table[slot, v, pl.ds(start + t, 8), :], lane),
                        total[v],
                    )
                    for v in range(9)
                ]
            for v in range(9):
                beside[f * 9 + v, rows, :] = total[v]

    def update(slot, h):
        rows = pl.ds(pl.multiple_of(8 * h, 8), 8)
        own = pl.ds(pl.multiple_of(16 + 8 * h, 8), 8)
        total = [jnp.zeros((8, LANES), jnp.float32) for i in range(9)]
        for f in range(3):
            for j in range(9):
                near = beside[f * 9 + j, rows, :]
                total = [total[i] + matrix(9 + 9 * f, i, j, h) * near for i in range(9)]
        remain = [
            rhs[pl.ds(pl.multiple_of(i * 16 + h * 8, 8), 8), :] - total[i] for i in range(9)
        ]
        for i, change in enumerate(apply_inverse(remain, h)):
            now = table[slot, i, own, :]
            table[slot + 1, i, own, :] = (1.0 - damping) * now + damping * change

    early = jnp.where(d < half, 0, 1)
    late = 1 - early

    def sweep(slot, carry):
        for h in range(2):
            pick(slot, h, 16, 16 - 8 * h, 9, False)
        for s in (early, late):
            if s is late:

                @pl.when(jnp.logical_and(fed, slot == 0))
                def _():
                    for b in range(N_GRP):
                        feed_copy(0, b).wait_recv()
                    for b in range(N_GRP):
                        for v in range(9):
                            table[0, v, b : b + 1, :] = feed[b, v : v + 1, :]

            arrive(slot, s, False)
            for h in range(2):
                pick(slot, h, 8 + 17 * s, 8 + 17 * s - 8 * h, 8, True)
            if s is late:
                update(slot, early)
            arrive(slot, s, True)
            pick(slot, s, 33 * s, 25 * s, 8, True)
        update(slot, late)

        @pl.when(slot < SWEEPS - 3)
        def _():
            each_send(slot + 1, lambda copy: copy.start())

        @pl.when(slot == SWEEPS - 3)
        def _():
            each_send(slot + 1, lambda copy: copy.start(), True)

        return carry

    lax.fori_loop(0, SWEEPS - 2, sweep, 0)

    last = SWEEPS - 2
    sublane = lax.broadcasted_iota(jnp.int32, (8, LANES), 0)
    mine = pl.ds(g, 1)

    def pick_last(tiles, resume):
        for f in range(3):
            lane = jnp.broadcast_to(lane_idx[f, mine, :], (8, LANES))
            block = jnp.broadcast_to(block_idx[f, mine, :], (8, LANES))
            block = jnp.where(block < 0, -1, block + g - sublane)
            if resume:
                total = [beside[f * 9 + v, 0:8, :] for v in range(9)]
            else:
                total = [jnp.zeros((8, LANES), jnp.float32) for v in range(9)]
            for tile in tiles:
                rows = pl.ds(pl.multiple_of(8 * tile, 8), 8)
                mask = block == 8 * tile
                total = [
                    jnp.where(mask, gathered(table[last, v, rows, :], lane), total[v])
                    for v in range(9)
                ]
            for v in range(9):
                beside[f * 9 + v, 0:8, :] = total[v]

    pick_last((2, 3), False)
    for v in range(9):
        final[0, v : v + 1, :] = table[last, v, pl.ds(16 + g, 1), :]
    for s in (early, late):
        arrive(last, s, False)
        pick_last((1 + 3 * s,), True)
        arrive(last, s, True)
        pick_last((5 * s,), True)
    coupled = jnp.zeros((9, LANES), jnp.float32)
    for f in range(3):
        for j in range(9):
            near = jnp.sum(beside[f * 9 + j, 0:8, :], axis=0, keepdims=True)
            coupled = coupled + dense[pl.ds((9 + 9 * f) * 144 + j * 16 + g, 9, stride=144), :] * near
    final[1, 0:9, :] = rhs[pl.ds(g, 9, stride=16), :] - coupled
    change = jnp.zeros((9, LANES), jnp.float32)
    for j in range(9):
        change = change + dense[pl.ds(j * 16 + g, 9, stride=144), :] * final[1, j : j + 1, :]
    final[2, 0:9, :] = (1.0 - damping) * final[0, 0:9, :] + damping * change
    coarse = [final[2, pl.ds(m, 3, stride=3), :] for m in range(3)]
    for n in range(15):
        value = sum(pmat_ref[m, n] * coarse[m] for m in range(3))
        for v in range(3):
            out_ref[v, n : n + 1, :] = value[v : v + 1, :]

    for step in range(1, N_GRP):
        peer = lax.rem(g + step, N_GRP)
        rhs_copy(peer, g).wait_send()
    for slot in range(SWEEPS - 1):
        each_send(slot, lambda copy: copy.wait_send())

    @pl.when(feeding)
    def _():
        for k in range(len(leads)):
            feed_copy(k, g).wait_send()


def solution(mesh):
    n_dom = mesh.shape["dom"]

    def local(
        fine_level_residual,
        restriction_matrix,
        prolongation_matrix,
        block_inverse,
        face_coupling,
        neighbours,
    ):
        width = block_inverse.shape[2]
        call = pl.pallas_call(
            lambda *refs: kernel(n_dom, *refs),
            out_shape=jax.ShapeDtypeStruct((3, 15, LANES), jnp.float32),
            in_specs=[pl.BlockSpec(memory_space=pl.ANY)] * 6,
            out_specs=pl.BlockSpec(memory_space=pltpu.VMEM),
            scratch_shapes=[
                pltpu.VMEM((3, 15, LANES), jnp.float32),
                pltpu.SMEM((3, 15), jnp.float32),
                pltpu.SMEM((3, 15), jnp.float32),
                pltpu.VMEM((3, width), jnp.int32),
                pltpu.VMEM((9, 9, width), jnp.bfloat16),
                pltpu.VMEM((81, 3, width), jnp.bfloat16),
                pltpu.VMEM((36 * 144, LANES), jnp.float32),
                pltpu.VMEM((3, 16, LANES), jnp.int32),
                pltpu.VMEM((3, 16, LANES), jnp.int32),
                pltpu.VMEM((9, LANES), jnp.float32),
                pltpu.VMEM((16, 9, LANES), jnp.float32),
                pltpu.VMEM((144, LANES), jnp.float32),
                pltpu.VMEM((SWEEPS - 1, 9, 48, LANES), jnp.float32),
                pltpu.VMEM((27, 16, LANES), jnp.float32),
                pltpu.VMEM((3, 16, LANES), jnp.float32),
                pltpu.VMEM((9, LANES), jnp.float32),
                pltpu.VMEM((16, 9, LANES), jnp.float32),
                pltpu.SemaphoreType.DMA((6,)),
                pltpu.SemaphoreType.DMA((16,)),
                pltpu.SemaphoreType.DMA((16,)),
                pltpu.SemaphoreType.DMA((SWEEPS - 1, 8)),
                pltpu.SemaphoreType.DMA((SWEEPS - 1, 4)),
                pltpu.SemaphoreType.DMA((8,)),
                pltpu.SemaphoreType.DMA((16,)),
                pltpu.SemaphoreType.REGULAR,
            ],
            compiler_params=pltpu.CompilerParams(collective_id=0, has_side_effects=True),
            name="jacobi",
        )
        return call(
            fine_level_residual,
            restriction_matrix,
            prolongation_matrix.T,
            neighbours,
            block_inverse,
            face_coupling.transpose(1, 2, 0, 3).reshape(81, 3, width),
        )

    placed = (
        P(None, None, ("dom", "grp")),
        P(),
        P(),
        P(None, None, "dom"),
        P(None, None, None, "dom"),
        P(None, "dom"),
    )
    return jax.shard_map(
        local, mesh=mesh, in_specs=placed, out_specs=P(None, None, ("dom", "grp")), check_vma=False
    )
```

```python
import jax
import jax.numpy as jnp
from jax import lax
from jax.experimental import pallas as pl
from jax.experimental.pallas import tpu as pltpu
from jax.sharding import PartitionSpec as P

SWEEPS = 6
MESH = pl.DeviceIdType.MESH
damping = 0.8
N_GRP = 16
LANES = 128


def gathered(x, lane):
    return jnp.take_along_axis(x, lane, axis=1, mode="promise_in_bounds")


def kernel(
    n_dom,
    res_hbm,
    rmat_hbm,
    pmat_hbm,
    nb_hbm,
    inv_hbm,
    cpl_hbm,
    out_ref,
    res_ref,
    rmat_ref,
    pmat_ref,
    nb_ref,
    inv_v,
    cpl_v,
    dense,
    lane_idx,
    block_idx,
    own_rhs,
    land,
    rhs,
    table,
    beside,
    final,
    feed_own,
    feed,
    load_sem,
    gsend,
    grecv,
    hsend,
    hrecv,
    fsend,
    frecv,
    ready,
    ready_high,
    group_ready,
):
    d = lax.axis_index("dom")
    g = lax.axis_index("grp")
    half = n_dom // 2
    column, row = g // 4 * 4, g % 4
    lead = jnp.logical_or(row == 0, row == 3)
    cross_low, cross_high = d == half, d == half - 1
    has = (d > 0, d < n_dom - 1)
    cross = (cross_low, cross_high)
    first_row = 3 - row
    second_row = jnp.where(row == 3, 1, 2)
    source_row = jnp.where(row < 2, 3, 0)
    side_dom = (d - 1, d + 1)
    first = [jnp.where(cross[s], column + first_row, g) for s in range(2)]
    second = column + second_row
    source = [jnp.where(cross[s], column + source_row, g) for s in range(2)]
    sends = [
        jnp.logical_and(has[s], jnp.logical_or(jnp.logical_not(cross[s]), lead)) for s in range(2)
    ]
    twice = [jnp.logical_and(cross[s], lead) for s in range(2)]
    feeding, fed = cross_high, jnp.logical_and(cross_low, lead)
    leads = [4 * x + y for x in range(4) for y in (3, 0)]

    loads = [
        pltpu.make_async_copy(src, dst, load_sem.at[i])
        for i, (src, dst) in enumerate(
            (
                (res_hbm, res_ref),
                (rmat_hbm, rmat_ref),
                (pmat_hbm, pmat_ref),
                (nb_hbm, nb_ref),
                (inv_hbm, inv_v),
                (cpl_hbm, cpl_v),
            )
        )
    ]
    for load in loads:
        load.start()

    early = jnp.where(d < half, 0, 1)
    late = 1 - early
    barrier = pltpu.get_barrier_semaphore()
    order = [0, 4, 1, 12, 8, 5, 2, 13, 9, 6, 3, 14, 10, 7, 15, 11]
    rank = sum(jnp.where(g == device, k, 0) for k, device in enumerate(order))

    for k, peer in enumerate(order):

        @pl.when(jnp.where(feeding, k > rank, k != rank))
        def _():
            pl.semaphore_signal(barrier, inc=1, device_id=(d, peer), device_id_type=MESH)
    answers_low = d == half + 1
    for s in range(2):
        silent = feeding if s else jnp.logical_or(fed, answers_low)

        @pl.when(jnp.logical_and(has[s], jnp.logical_not(silent)))
        def _():
            pl.semaphore_signal(
                barrier, inc=1, device_id=(side_dom[s], source[s]), device_id_type=MESH
            )

    @pl.when(fed)
    def _():
        for other in range(N_GRP):
            pl.semaphore_signal(barrier, inc=1, device_id=(d - 1, other), device_id_type=MESH)

    low = jnp.logical_and(sends[0], jnp.logical_not(cross_low))
    high = jnp.logical_and(sends[1], jnp.logical_not(cross_low))
    signals = jnp.where(feeding, rank + len(leads), N_GRP - 1 + high.astype(jnp.int32))
    signals = signals + low.astype(jnp.int32) + twice[1].astype(jnp.int32)

    @pl.when(feeding)
    def _():
        pl.semaphore_wait(barrier, signals)
        for k, peer in enumerate(order):

            @pl.when(k < rank)
            def _():
                pl.semaphore_signal(
                    group_ready, inc=1, device_id=(d, peer), device_id_type=MESH
                )

        pl.semaphore_signal(
            ready, inc=1, device_id=(side_dom[1], source[1]), device_id_type=MESH
        )

    loads[0].wait()
    loads[1].wait()
    for m in range(3):
        total = jnp.zeros((3, LANES), jnp.float32)
        for n in range(15):
            total = total + rmat_ref[m, n] * res_ref[:, n, :]
        for v in range(3):
            own_rhs[3 * v + m : 3 * v + m + 1, :] = total[v : v + 1, :]

    @pl.when(jnp.logical_not(feeding))
    def _():
        pl.semaphore_wait(barrier, signals)

    @pl.when(answers_low)
    def _():
        pl.semaphore_signal(ready_high, inc=1, device_id=(d - 1, g), device_id_type=MESH)

    def rhs_copy(peer, owner):
        return pltpu.make_async_remote_copy(
            src_ref=own_rhs,
            dst_ref=land.at[owner],
            send_sem=gsend.at[peer],
            recv_sem=grecv.at[owner],
            device_id=(d, peer),
            device_id_type=MESH,
        )

    def feed_copy(k, owner):
        return pltpu.make_async_remote_copy(
            src_ref=feed_own,
            dst_ref=feed.at[owner],
            send_sem=fsend.at[k],
            recv_sem=frecv.at[owner],
            device_id=(d + 1, leads[k]),
            device_id_type=MESH,
        )

    @pl.when(feeding)
    def _():
        loads[4].wait()
        own = pl.ds(pl.multiple_of(g * LANES, LANES), LANES)
        for i in range(9):
            part = inv_v[i, :, own].astype(jnp.float32) * own_rhs[...]
            feed_own[i : i + 1, :] = damping * jnp.sum(part, axis=0, keepdims=True)
        for k in range(len(leads)):
            feed_copy(k, g).start()

    @pl.when(jnp.logical_and(feeding, rank < N_GRP - 1))
    def _():
        pl.semaphore_wait(group_ready, N_GRP - 1 - rank)

    for step in range(1, N_GRP):
        peer = lax.rem(g + step, N_GRP)
        rhs_copy(peer, g).start()

    loads[2].wait()
    loads[3].wait()
    for f in range(3):
        for b in range(N_GRP):
            lane_idx[f, b : b + 1, :] = nb_ref[f : f + 1, b * LANES : (b + 1) * LANES]
        offsets = lane_idx[f]
        lanes = lax.broadcasted_iota(jnp.int32, (N_GRP, LANES), 1)
        position = offsets + lanes + N_GRP * LANES
        block_idx[f] = jnp.where(offsets != 0, lax.shift_right_arithmetic(position, 7), -1)
        lane_idx[f] = jnp.bitwise_and(position, LANES - 1)

    @pl.when(jnp.logical_not(feeding))
    def _():
        loads[4].wait()


    def spread_inv(i, carry):
        for b in range(N_GRP):
            tile = inv_v[i, :, b * LANES : (b + 1) * LANES].astype(jnp.float32)
            dense[pl.ds(i * 144 + b, 9, stride=16), :] = tile
        return carry

    lax.fori_loop(0, 9, spread_inv, 0)
    loads[5].wait()

    def spread_cpl(ij, carry):
        for b in range(N_GRP):
            tile = cpl_v[ij, :, b * LANES : (b + 1) * LANES].astype(jnp.float32)
            dense[pl.ds(1296 + ij * 16 + b, 3, stride=1296), :] = tile
        return carry

    lax.fori_loop(0, 81, spread_cpl, 0)

    land[g] = own_rhs[...]
    for step in range(1, N_GRP):
        peer = lax.rem(g + step, N_GRP)
        rhs_copy(peer, peer).wait_recv()
    for b in range(N_GRP):
        rhs[pl.ds(b, 9, stride=16), :] = land[b]

    def matrix(base, i, j, h):
        start = (base + i) * 144 + j * 16 + h * 8
        return dense[pl.ds(start if isinstance(h, int) else pl.multiple_of(start, 8), 8), :]

    def apply_inverse(remain, h):
        result = [matrix(0, i, 0, h) * remain[0] for i in range(9)]
        for j in range(1, 9):
            result = [result[i] + matrix(0, i, j, h) * remain[j] for i in range(9)]
        return result

    for h in range(2):
        remain = [rhs[j * 16 + h * 8 : j * 16 + h * 8 + 8, :] for j in range(9)]
        for i, update in enumerate(apply_inverse(remain, h)):
            table[0, i, 16 + 8 * h : 24 + 8 * h, :] = damping * update

    def halo(slot, s, which, h):
        own, there = 16 + 8 * h, (32 if s == 0 else 0) + 8 * h
        return pltpu.make_async_remote_copy(
            src_ref=table.at[slot, :, own : own + 8, :],
            dst_ref=table.at[slot, :, there : there + 8, :],
            send_sem=hsend.at[slot, 4 * s + 2 * which + h],
            recv_sem=hrecv.at[slot, 2 * (1 - s) + h],
            device_id=(side_dom[s], second if which else first[s]),
            device_id_type=MESH,
        )

    def each_send(slot, act, sides=(0, 1)):
        for which, flags in ((0, sends), (1, twice)):
            for s in sides:
                flag = flags[s]
                if isinstance(slot, int) and slot == 0 and s == 1 and which == 0:
                    flag = jnp.logical_and(flag, jnp.logical_not(feeding))

                @pl.when(flag)
                def _():
                    act(halo(slot, s, which, s))
                    act(halo(slot, s, which, 1 - s))

    @pl.when(fed)
    def _():
        pl.semaphore_wait(ready, 2)

    each_send(0, lambda copy: copy.start(), sides=(0,))

    @pl.when(cross_low)
    def _():
        pl.semaphore_wait(ready_high, 1)

    each_send(0, lambda copy: copy.start(), sides=(1,))

    def send_half(slot, part):
        for s in range(2):

            @pl.when(jnp.logical_and(late == s, jnp.logical_and(twice[s], slot == SWEEPS - 2)))
            def _():
                halo(slot, s, 1, 1 - s if part else s).start()

            @pl.when(jnp.logical_and(late == s, sends[s]))
            def _():
                halo(slot, s, 0, 1 - s if part else s).start()

        if part:
            for s in range(2):

                @pl.when(jnp.logical_and(early == s, sends[s]))
                def _():
                    halo(slot, s, 0, s).start()
                    halo(slot, s, 0, 1 - s).start()

            for s in range(2):

                @pl.when(jnp.logical_and(late == s, jnp.logical_and(twice[s], slot < SWEEPS - 2)))
                def _():
                    halo(slot, s, 1, s).start()
                    halo(slot, s, 1, 1 - s).start()

    def arrive(slot, s, far):
        for low in range(2):

            due = jnp.logical_and(s == low, has[low])
            if low == 0 and not isinstance(slot, int):
                due = jnp.logical_and(due, jnp.logical_not(jnp.logical_and(fed, slot == 0)))

            @pl.when(due)
            def _():
                halo(slot, 1 - low, 0, low if far else 1 - low).wait_recv()

    def pick(slot, h, start, k_start, count, resume):
        rows = pl.ds(pl.multiple_of(8 * h, 8), 8)
        for f in range(3):
            lane = lane_idx[f, rows, :]
            block = block_idx[f, rows, :] - k_start
            if resume:
                total = [beside[f * 9 + v, rows, :] for v in range(9)]
            else:
                total = [jnp.zeros((8, LANES), jnp.float32) for v in range(9)]
            for t in range(count):
                mask = block == t
                total = [
                    jnp.where(
                        mask,
                        gathered(table[slot, v, pl.ds(start + t, 8), :], lane),
                        total[v],
                    )
                    for v in range(9)
                ]
            for v in range(9):
                beside[f * 9 + v, rows, :] = total[v]

    def update(slot, h):
        rows = pl.ds(pl.multiple_of(8 * h, 8), 8)
        own = pl.ds(pl.multiple_of(16 + 8 * h, 8), 8)
        total = [jnp.zeros((8, LANES), jnp.float32) for i in range(9)]
        for f in range(3):
            for j in range(9):
                near = beside[f * 9 + j, rows, :]
                total = [total[i] + matrix(9 + 9 * f, i, j, h) * near for i in range(9)]
        remain = [
            rhs[pl.ds(pl.multiple_of(i * 16 + h * 8, 8), 8), :] - total[i] for i in range(9)
        ]
        for i, change in enumerate(apply_inverse(remain, h)):
            now = table[slot, i, own, :]
            table[slot + 1, i, own, :] = (1.0 - damping) * now + damping * change

    def sweep(slot, carry):
        for h in range(2):
            pick(slot, h, 16, 16 - 8 * h, 9, False)
        arrive(slot, early, False)
        for h in range(2):
            pick(slot, h, 8 + 17 * early, 8 + 17 * early - 8 * h, 8, True)
        arrive(slot, early, True)
        pick(slot, early, 33 * early, 25 * early, 8, True)

        @pl.when(jnp.logical_and(fed, slot == 0))
        def _():
            for b in range(N_GRP):
                feed_copy(0, b).wait_recv()
            for b in range(N_GRP):
                for v in range(9):
                    table[0, v, b : b + 1, :] = feed[b, v : v + 1, :]

        arrive(slot, late, False)
        pick(slot, late, 8 + 17 * late, 8 + 9 * late, 8, True)
        arrive(slot, late, True)
        pick(slot, late, 33 * late, 25 * late, 8, True)
        update(slot, late)
        send_half(slot + 1, 0)
        pick(slot, early, 8 + 17 * late, 25 * late, 8, True)
        update(slot, early)
        send_half(slot + 1, 1)
        return carry

    lax.fori_loop(0, SWEEPS - 2, sweep, 0)

    last = SWEEPS - 2
    sublane = lax.broadcasted_iota(jnp.int32, (8, LANES), 0)
    mine = pl.ds(g, 1)

    def pick_last(tiles, resume):
        for f in range(3):
            lane = jnp.broadcast_to(lane_idx[f, mine, :], (8, LANES))
            block = jnp.broadcast_to(block_idx[f, mine, :], (8, LANES))
            block = jnp.where(block < 0, -1, block + g - sublane)
            if resume:
                total = [beside[f * 9 + v, 0:8, :] for v in range(9)]
            else:
                total = [jnp.zeros((8, LANES), jnp.float32) for v in range(9)]
            for tile in tiles:
                rows = pl.ds(pl.multiple_of(8 * tile, 8), 8)
                mask = block == 8 * tile
                total = [
                    jnp.where(mask, gathered(table[last, v, rows, :], lane), total[v])
                    for v in range(9)
                ]
            for v in range(9):
                beside[f * 9 + v, 0:8, :] = total[v]

    pick_last((2, 3), False)
    for v in range(9):
        final[0, v : v + 1, :] = table[last, v, pl.ds(16 + g, 1), :]
    for s in (early, late):
        arrive(last, s, False)
        pick_last((1 + 3 * s,), True)
        arrive(last, s, True)
        pick_last((5 * s,), True)
    coupled = jnp.zeros((9, LANES), jnp.float32)
    for f in range(3):
        for j in range(9):
            near = jnp.sum(beside[f * 9 + j, 0:8, :], axis=0, keepdims=True)
            coupled = coupled + dense[pl.ds((9 + 9 * f) * 144 + j * 16 + g, 9, stride=144), :] * near
    final[1, 0:9, :] = rhs[pl.ds(g, 9, stride=16), :] - coupled
    change = jnp.zeros((9, LANES), jnp.float32)
    for j in range(9):
        change = change + dense[pl.ds(j * 16 + g, 9, stride=144), :] * final[1, j : j + 1, :]
    final[2, 0:9, :] = (1.0 - damping) * final[0, 0:9, :] + damping * change
    coarse = [final[2, pl.ds(m, 3, stride=3), :] for m in range(3)]
    for n in range(15):
        value = sum(pmat_ref[m, n] * coarse[m] for m in range(3))
        for v in range(3):
            out_ref[v, n : n + 1, :] = value[v : v + 1, :]

    for step in range(1, N_GRP):
        peer = lax.rem(g + step, N_GRP)
        rhs_copy(peer, g).wait_send()
    for slot in range(SWEEPS - 1):
        each_send(slot, lambda copy: copy.wait_send())

    @pl.when(feeding)
    def _():
        for k in range(len(leads)):
            feed_copy(k, g).wait_send()


def solution(mesh):
    n_dom = mesh.shape["dom"]

    def local(
        fine_level_residual,
        restriction_matrix,
        prolongation_matrix,
        block_inverse,
        face_coupling,
        neighbours,
    ):
        width = block_inverse.shape[2]
        call = pl.pallas_call(
            lambda *refs: kernel(n_dom, *refs),
            out_shape=jax.ShapeDtypeStruct((3, 15, LANES), jnp.float32),
            in_specs=[pl.BlockSpec(memory_space=pl.ANY)] * 6,
            out_specs=pl.BlockSpec(memory_space=pltpu.VMEM),
            scratch_shapes=[
                pltpu.VMEM((3, 15, LANES), jnp.float32),
                pltpu.SMEM((3, 15), jnp.float32),
                pltpu.SMEM((3, 15), jnp.float32),
                pltpu.VMEM((3, width), jnp.int32),
                pltpu.VMEM((9, 9, width), jnp.bfloat16),
                pltpu.VMEM((81, 3, width), jnp.bfloat16),
                pltpu.VMEM((36 * 144, LANES), jnp.float32),
                pltpu.VMEM((3, 16, LANES), jnp.int32),
                pltpu.VMEM((3, 16, LANES), jnp.int32),
                pltpu.VMEM((9, LANES), jnp.float32),
                pltpu.VMEM((16, 9, LANES), jnp.float32),
                pltpu.VMEM((144, LANES), jnp.float32),
                pltpu.VMEM((SWEEPS - 1, 9, 48, LANES), jnp.float32),
                pltpu.VMEM((27, 16, LANES), jnp.float32),
                pltpu.VMEM((3, 16, LANES), jnp.float32),
                pltpu.VMEM((9, LANES), jnp.float32),
                pltpu.VMEM((16, 9, LANES), jnp.float32),
                pltpu.SemaphoreType.DMA((6,)),
                pltpu.SemaphoreType.DMA((16,)),
                pltpu.SemaphoreType.DMA((16,)),
                pltpu.SemaphoreType.DMA((SWEEPS - 1, 8)),
                pltpu.SemaphoreType.DMA((SWEEPS - 1, 4)),
                pltpu.SemaphoreType.DMA((8,)),
                pltpu.SemaphoreType.DMA((16,)),
                pltpu.SemaphoreType.REGULAR,
                pltpu.SemaphoreType.REGULAR,
                pltpu.SemaphoreType.REGULAR,
            ],
            compiler_params=pltpu.CompilerParams(collective_id=0, has_side_effects=True),
            name="jacobi",
        )
        return call(
            fine_level_residual,
            restriction_matrix,
            prolongation_matrix.T,
            neighbours,
            block_inverse,
            face_coupling.transpose(1, 2, 0, 3).reshape(81, 3, width),
        )

    placed = (
        P(None, None, ("dom", "grp")),
        P(),
        P(),
        P(None, None, "dom"),
        P(None, None, None, "dom"),
        P(None, "dom"),
    )
    return jax.shard_map(
        local, mesh=mesh, in_specs=placed, out_specs=P(None, None, ("dom", "grp")), check_vma=False
    )
```

```python
import jax
import jax.numpy as jnp
from jax import lax
from jax.experimental import pallas as pl
from jax.experimental.pallas import tpu as pltpu
from jax.sharding import PartitionSpec as P

SWEEPS = 6
MESH = pl.DeviceIdType.MESH
damping = 0.8
N_GRP = 16
LANES = 128


def gathered(x, lane):
    return jnp.take_along_axis(x, lane, axis=1, mode="promise_in_bounds")


def kernel(
    n_dom,
    res_hbm,
    rmat_hbm,
    pmat_hbm,
    nb_hbm,
    inv_hbm,
    cpl_hbm,
    out_ref,
    res_ref,
    rmat_ref,
    pmat_ref,
    nb_ref,
    inv_v,
    cpl_v,
    dense,
    lane_idx,
    block_idx,
    own_rhs,
    land,
    rhs,
    table,
    beside,
    final,
    feed_own,
    feed,
    load_sem,
    gsend,
    grecv,
    hsend,
    hrecv,
    fsend,
    frecv,
    ready,
    ready_high,
    group_ready,
):
    d = lax.axis_index("dom")
    g = lax.axis_index("grp")
    half = n_dom // 2
    column, row = g // 4 * 4, g % 4
    lead = jnp.logical_or(row == 0, row == 3)
    cross_low, cross_high = d == half, d == half - 1
    has = (d > 0, d < n_dom - 1)
    cross = (cross_low, cross_high)
    first_row = 3 - row
    second_row = jnp.where(row == 3, 1, 2)
    source_row = jnp.where(row < 2, 3, 0)
    side_dom = (d - 1, d + 1)
    first = [jnp.where(cross[s], column + first_row, g) for s in range(2)]
    second = column + second_row
    source = [jnp.where(cross[s], column + source_row, g) for s in range(2)]
    sends = [
        jnp.logical_and(has[s], jnp.logical_or(jnp.logical_not(cross[s]), lead)) for s in range(2)
    ]
    twice = [jnp.logical_and(cross[s], lead) for s in range(2)]
    feeding, fed = cross_high, jnp.logical_and(cross_low, lead)
    leads = [4 * x + y for x in range(4) for y in (3, 0)]

    loads = [
        pltpu.make_async_copy(src, dst, load_sem.at[i])
        for i, (src, dst) in enumerate(
            (
                (res_hbm, res_ref),
                (rmat_hbm, rmat_ref),
                (pmat_hbm, pmat_ref),
                (nb_hbm, nb_ref),
                (inv_hbm, inv_v),
                (cpl_hbm, cpl_v),
            )
        )
    ]
    for load in loads:
        load.start()

    early = jnp.where(d < half, 0, 1)
    late = 1 - early
    barrier = pltpu.get_barrier_semaphore()
    order = [0, 4, 1, 12, 8, 5, 2, 13, 9, 6, 3, 14, 10, 7, 15, 11]
    rank = sum(jnp.where(g == device, k, 0) for k, device in enumerate(order))

    for k, peer in enumerate(order):

        @pl.when(jnp.where(feeding, k > rank, k != rank))
        def _():
            pl.semaphore_signal(barrier, inc=1, device_id=(d, peer), device_id_type=MESH)
    answers_low = d == half + 1
    for s in range(2):
        silent = feeding if s else jnp.logical_or(fed, answers_low)

        @pl.when(jnp.logical_and(has[s], jnp.logical_not(silent)))
        def _():
            pl.semaphore_signal(
                barrier, inc=1, device_id=(side_dom[s], source[s]), device_id_type=MESH
            )

    @pl.when(fed)
    def _():
        for other in range(N_GRP):
            pl.semaphore_signal(barrier, inc=1, device_id=(d - 1, other), device_id_type=MESH)

    low = jnp.logical_and(sends[0], jnp.logical_not(cross_low))
    high = jnp.logical_and(sends[1], jnp.logical_not(cross_low))
    signals = jnp.where(feeding, rank + len(leads), N_GRP - 1 + high.astype(jnp.int32))
    signals = signals + low.astype(jnp.int32) + twice[1].astype(jnp.int32)

    @pl.when(feeding)
    def _():
        pl.semaphore_wait(barrier, signals)
        for k, peer in enumerate(order):

            @pl.when(k < rank)
            def _():
                pl.semaphore_signal(
                    group_ready, inc=1, device_id=(d, peer), device_id_type=MESH
                )

        pl.semaphore_signal(
            ready, inc=1, device_id=(side_dom[1], source[1]), device_id_type=MESH
        )

    loads[0].wait()
    loads[1].wait()
    for m in range(3):
        total = jnp.zeros((3, LANES), jnp.float32)
        for n in range(15):
            total = total + rmat_ref[m, n] * res_ref[:, n, :]
        for v in range(3):
            own_rhs[3 * v + m : 3 * v + m + 1, :] = total[v : v + 1, :]

    @pl.when(jnp.logical_not(feeding))
    def _():
        pl.semaphore_wait(barrier, signals)

    @pl.when(answers_low)
    def _():
        pl.semaphore_signal(ready_high, inc=1, device_id=(d - 1, g), device_id_type=MESH)

    def rhs_copy(peer, owner):
        return pltpu.make_async_remote_copy(
            src_ref=own_rhs,
            dst_ref=land.at[owner],
            send_sem=gsend.at[peer],
            recv_sem=grecv.at[owner],
            device_id=(d, peer),
            device_id_type=MESH,
        )

    def feed_copy(k, owner):
        return pltpu.make_async_remote_copy(
            src_ref=feed_own,
            dst_ref=feed.at[owner],
            send_sem=fsend.at[k],
            recv_sem=frecv.at[owner],
            device_id=(d + 1, leads[k]),
            device_id_type=MESH,
        )

    @pl.when(feeding)
    def _():
        loads[4].wait()
        own = pl.ds(pl.multiple_of(g * LANES, LANES), LANES)
        for i in range(9):
            part = inv_v[i, :, own].astype(jnp.float32) * own_rhs[...]
            feed_own[i : i + 1, :] = damping * jnp.sum(part, axis=0, keepdims=True)
        for k in range(len(leads)):
            feed_copy(k, g).start()

    @pl.when(jnp.logical_and(feeding, rank < N_GRP - 1))
    def _():
        pl.semaphore_wait(group_ready, N_GRP - 1 - rank)

    for step in range(1, N_GRP):
        peer = lax.rem(g + step, N_GRP)
        rhs_copy(peer, g).start()

    loads[2].wait()
    loads[3].wait()
    for f in range(3):
        for b in range(N_GRP):
            lane_idx[f, b : b + 1, :] = nb_ref[f : f + 1, b * LANES : (b + 1) * LANES]
        offsets = lane_idx[f]
        lanes = lax.broadcasted_iota(jnp.int32, (N_GRP, LANES), 1)
        position = offsets + lanes + N_GRP * LANES
        block_idx[f] = jnp.where(offsets != 0, lax.shift_right_arithmetic(position, 7), -1)
        lane_idx[f] = jnp.bitwise_and(position, LANES - 1)

    @pl.when(jnp.logical_not(feeding))
    def _():
        loads[4].wait()


    def spread_inv(i, carry):
        for b in range(N_GRP):
            tile = inv_v[i, :, b * LANES : (b + 1) * LANES].astype(jnp.float32)
            dense[pl.ds(i * 144 + b, 9, stride=16), :] = tile
        return carry

    lax.fori_loop(0, 9, spread_inv, 0)
    loads[5].wait()

    def spread_cpl(ij, carry):
        for b in range(N_GRP):
            tile = cpl_v[ij, :, b * LANES : (b + 1) * LANES].astype(jnp.float32)
            dense[pl.ds(1296 + ij * 16 + b, 3, stride=1296), :] = tile
        return carry

    lax.fori_loop(0, 81, spread_cpl, 0)

    land[g] = own_rhs[...]
    for step in range(1, N_GRP):
        peer = lax.rem(g + step, N_GRP)
        rhs_copy(peer, peer).wait_recv()
    for b in range(N_GRP):
        rhs[pl.ds(b, 9, stride=16), :] = land[b]

    def matrix(base, i, j, h):
        start = (base + i) * 144 + j * 16 + h * 8
        return dense[pl.ds(start if isinstance(h, int) else pl.multiple_of(start, 8), 8), :]

    def apply_inverse(remain, h):
        result = [matrix(0, i, 0, h) * remain[0] for i in range(9)]
        for j in range(1, 9):
            result = [result[i] + matrix(0, i, j, h) * remain[j] for i in range(9)]
        return result

    for h in range(2):
        remain = [rhs[j * 16 + h * 8 : j * 16 + h * 8 + 8, :] for j in range(9)]
        for i, update in enumerate(apply_inverse(remain, h)):
            table[0, i, 16 + 8 * h : 24 + 8 * h, :] = damping * update

    def halo(slot, s, which, h):
        own, there = 16 + 8 * h, (32 if s == 0 else 0) + 8 * h
        return pltpu.make_async_remote_copy(
            src_ref=table.at[slot, :, own : own + 8, :],
            dst_ref=table.at[slot, :, there : there + 8, :],
            send_sem=hsend.at[slot, 4 * s + 2 * which + h],
            recv_sem=hrecv.at[slot, 2 * (1 - s) + h],
            device_id=(side_dom[s], second if which else first[s]),
            device_id_type=MESH,
        )

    def each_send(slot, act, sides=(0, 1)):
        for which, flags in ((0, sends), (1, twice)):
            for s in sides:
                flag = flags[s]
                if isinstance(slot, int) and slot == 0 and s == 1 and which == 0:
                    flag = jnp.logical_and(flag, jnp.logical_not(feeding))

                @pl.when(flag)
                def _():
                    act(halo(slot, s, which, s))
                    act(halo(slot, s, which, 1 - s))

    @pl.when(fed)
    def _():
        pl.semaphore_wait(ready, 2)

    each_send(0, lambda copy: copy.start(), sides=(0,))

    @pl.when(cross_low)
    def _():
        pl.semaphore_wait(ready_high, 1)

    each_send(0, lambda copy: copy.start(), sides=(1,))

    def send_half(slot, part):
        for s in range(2):

            @pl.when(jnp.logical_and(late == s, jnp.logical_and(twice[s], slot == SWEEPS - 2)))
            def _():
                halo(slot, s, 1, 1 - s if part else s).start()

            @pl.when(jnp.logical_and(late == s, sends[s]))
            def _():
                halo(slot, s, 0, 1 - s if part else s).start()

        if part:
            for s in range(2):

                @pl.when(jnp.logical_and(early == s, sends[s]))
                def _():
                    halo(slot, s, 0, s).start()
                    halo(slot, s, 0, 1 - s).start()

            for s in range(2):

                @pl.when(jnp.logical_and(late == s, jnp.logical_and(twice[s], slot < SWEEPS - 2)))
                def _():
                    halo(slot, s, 1, s).start()
                    halo(slot, s, 1, 1 - s).start()

    def arrive(slot, s, far):
        for low in range(2):

            due = jnp.logical_and(s == low, has[low])
            if low == 0 and not isinstance(slot, int):
                due = jnp.logical_and(due, jnp.logical_not(jnp.logical_and(fed, slot == 0)))

            @pl.when(due)
            def _():
                halo(slot, 1 - low, 0, low if far else 1 - low).wait_recv()

    def pick(slot, h, start, k_start, count, resume):
        rows = pl.ds(pl.multiple_of(8 * h, 8), 8)
        for f in range(3):
            lane = lane_idx[f, rows, :]
            block = block_idx[f, rows, :] - k_start
            if resume:
                total = [beside[f * 9 + v, rows, :] for v in range(9)]
            else:
                total = [jnp.zeros((8, LANES), jnp.float32) for v in range(9)]
            for t in range(count):
                mask = block == t
                total = [
                    jnp.where(
                        mask,
                        gathered(table[slot, v, pl.ds(start + t, 8), :], lane),
                        total[v],
                    )
                    for v in range(9)
                ]
            for v in range(9):
                beside[f * 9 + v, rows, :] = total[v]

    def update(slot, h):
        rows = pl.ds(pl.multiple_of(8 * h, 8), 8)
        own = pl.ds(pl.multiple_of(16 + 8 * h, 8), 8)
        total = [jnp.zeros((8, LANES), jnp.float32) for i in range(9)]
        for f in range(3):
            for j in range(9):
                near = beside[f * 9 + j, rows, :]
                total = [total[i] + matrix(9 + 9 * f, i, j, h) * near for i in range(9)]
        remain = [
            rhs[pl.ds(pl.multiple_of(i * 16 + h * 8, 8), 8), :] - total[i] for i in range(9)
        ]
        for i, change in enumerate(apply_inverse(remain, h)):
            now = table[slot, i, own, :]
            table[slot + 1, i, own, :] = (1.0 - damping) * now + damping * change

    def sweep(slot, carry):
        for h in range(2):
            pick(slot, h, 16, 16 - 8 * h, 9, False)
        fresh = jnp.logical_and(fed, slot == 0)

        @pl.when(fresh)
        def _():
            for b in order:
                feed_copy(0, b).wait_recv()
                for v in range(9):
                    table[0, v, b : b + 1, :] = feed[b, v : v + 1, :]
            pick(slot, late, 8 + 17 * late, 8 + 9 * late, 8, True)

        arrive(slot, early, False)
        for h in range(2):
            pick(slot, h, 8 + 17 * early, 8 + 17 * early - 8 * h, 8, True)
        arrive(slot, early, True)
        pick(slot, early, 33 * early, 25 * early, 8, True)

        arrive(slot, late, False)

        @pl.when(jnp.logical_not(fresh))
        def _():
            pick(slot, late, 8 + 17 * late, 8 + 9 * late, 8, True)

        arrive(slot, late, True)
        pick(slot, late, 33 * late, 25 * late, 8, True)
        update(slot, late)
        send_half(slot + 1, 0)
        pick(slot, early, 8 + 17 * late, 25 * late, 8, True)
        update(slot, early)
        send_half(slot + 1, 1)
        return carry

    lax.fori_loop(0, SWEEPS - 2, sweep, 0)

    last = SWEEPS - 2
    sublane = lax.broadcasted_iota(jnp.int32, (8, LANES), 0)
    mine = pl.ds(g, 1)

    def pick_last(tiles, resume):
        for f in range(3):
            lane = jnp.broadcast_to(lane_idx[f, mine, :], (8, LANES))
            block = jnp.broadcast_to(block_idx[f, mine, :], (8, LANES))
            block = jnp.where(block < 0, -1, block + g - sublane)
            if resume:
                total = [beside[f * 9 + v, 0:8, :] for v in range(9)]
            else:
                total = [jnp.zeros((8, LANES), jnp.float32) for v in range(9)]
            for tile in tiles:
                rows = pl.ds(pl.multiple_of(8 * tile, 8), 8)
                mask = block == 8 * tile
                total = [
                    jnp.where(mask, gathered(table[last, v, rows, :], lane), total[v])
                    for v in range(9)
                ]
            for v in range(9):
                beside[f * 9 + v, 0:8, :] = total[v]

    pick_last((2, 3), False)
    for v in range(9):
        final[0, v : v + 1, :] = table[last, v, pl.ds(16 + g, 1), :]
    for s in (early, late):
        arrive(last, s, False)
        pick_last((1 + 3 * s,), True)
        arrive(last, s, True)
        pick_last((5 * s,), True)
    coupled = jnp.zeros((9, LANES), jnp.float32)
    for f in range(3):
        for j in range(9):
            near = jnp.sum(beside[f * 9 + j, 0:8, :], axis=0, keepdims=True)
            coupled = coupled + dense[pl.ds((9 + 9 * f) * 144 + j * 16 + g, 9, stride=144), :] * near
    final[1, 0:9, :] = rhs[pl.ds(g, 9, stride=16), :] - coupled
    change = jnp.zeros((9, LANES), jnp.float32)
    for j in range(9):
        change = change + dense[pl.ds(j * 16 + g, 9, stride=144), :] * final[1, j : j + 1, :]
    final[2, 0:9, :] = (1.0 - damping) * final[0, 0:9, :] + damping * change
    coarse = [final[2, pl.ds(m, 3, stride=3), :] for m in range(3)]
    for n in range(15):
        value = sum(pmat_ref[m, n] * coarse[m] for m in range(3))
        for v in range(3):
            out_ref[v, n : n + 1, :] = value[v : v + 1, :]

    for step in range(1, N_GRP):
        peer = lax.rem(g + step, N_GRP)
        rhs_copy(peer, g).wait_send()
    for slot in range(SWEEPS - 1):
        each_send(slot, lambda copy: copy.wait_send())

    @pl.when(feeding)
    def _():
        for k in range(len(leads)):
            feed_copy(k, g).wait_send()


def solution(mesh):
    n_dom = mesh.shape["dom"]

    def local(
        fine_level_residual,
        restriction_matrix,
        prolongation_matrix,
        block_inverse,
        face_coupling,
        neighbours,
    ):
        width = block_inverse.shape[2]
        call = pl.pallas_call(
            lambda *refs: kernel(n_dom, *refs),
            out_shape=jax.ShapeDtypeStruct((3, 15, LANES), jnp.float32),
            in_specs=[pl.BlockSpec(memory_space=pl.ANY)] * 6,
            out_specs=pl.BlockSpec(memory_space=pltpu.VMEM),
            scratch_shapes=[
                pltpu.VMEM((3, 15, LANES), jnp.float32),
                pltpu.SMEM((3, 15), jnp.float32),
                pltpu.SMEM((3, 15), jnp.float32),
                pltpu.VMEM((3, width), jnp.int32),
                pltpu.VMEM((9, 9, width), jnp.bfloat16),
                pltpu.VMEM((81, 3, width), jnp.bfloat16),
                pltpu.VMEM((36 * 144, LANES), jnp.float32),
                pltpu.VMEM((3, 16, LANES), jnp.int32),
                pltpu.VMEM((3, 16, LANES), jnp.int32),
                pltpu.VMEM((9, LANES), jnp.float32),
                pltpu.VMEM((16, 9, LANES), jnp.float32),
                pltpu.VMEM((144, LANES), jnp.float32),
                pltpu.VMEM((SWEEPS - 1, 9, 48, LANES), jnp.float32),
                pltpu.VMEM((27, 16, LANES), jnp.float32),
                pltpu.VMEM((3, 16, LANES), jnp.float32),
                pltpu.VMEM((9, LANES), jnp.float32),
                pltpu.VMEM((16, 9, LANES), jnp.float32),
                pltpu.SemaphoreType.DMA((6,)),
                pltpu.SemaphoreType.DMA((16,)),
                pltpu.SemaphoreType.DMA((16,)),
                pltpu.SemaphoreType.DMA((SWEEPS - 1, 8)),
                pltpu.SemaphoreType.DMA((SWEEPS - 1, 4)),
                pltpu.SemaphoreType.DMA((8,)),
                pltpu.SemaphoreType.DMA((16,)),
                pltpu.SemaphoreType.REGULAR,
                pltpu.SemaphoreType.REGULAR,
                pltpu.SemaphoreType.REGULAR,
            ],
            compiler_params=pltpu.CompilerParams(collective_id=0, has_side_effects=True),
            name="jacobi",
        )
        return call(
            fine_level_residual,
            restriction_matrix,
            prolongation_matrix.T,
            neighbours,
            block_inverse,
            face_coupling.transpose(1, 2, 0, 3).reshape(81, 3, width),
        )

    placed = (
        P(None, None, ("dom", "grp")),
        P(),
        P(),
        P(None, None, "dom"),
        P(None, None, None, "dom"),
        P(None, "dom"),
    )
    return jax.shard_map(
        local, mesh=mesh, in_specs=placed, out_specs=P(None, None, ("dom", "grp")), check_vma=False
    )
```
